32 devices in a mesh: grp: 2 (over x), ma: 16 (over z, y, core).
Axes of the slice: x: 2, y: 2, z: 4, core: 2. Of those that a mesh axis runs over, the one named last changes fastest.
Arguments:
- tbar_alm: bfloat16 [128, 8, 2, 257], P('ma', 'grp'), parts along dimension 1, may hold values from -6 to 6
- twf_alm: bfloat16 [128, 8, 2, 257], P('ma', 'grp'), parts along dimension 1, may hold values from -6 to 6
- legendre: bfloat16 [128, 257, 16], P('ma'), may hold values from -0.375 to 0.375
- m_slots: int32 [128], replicated, may hold values from 0 to 127, each once
- cycle_order: int32 [16], replicated, may hold values from 0 to 15, each once
- colatitude: float32 [16], replicated, may hold values from 0.35 to 2.79
- cycle_weight: float32 [16], replicated, may hold values from 0.25 to 1
- pixel_mask: int32 [16, 4096], P('ma'), may hold values from 0 to 3
Outputs:
- gradient: float32 [128, 8, 2, 257], P('ma', 'grp'), parts along dimension 1
- curl: float32 [128, 8, 2, 257], P('ma', 'grp'), parts along dimension 1
The draws below stay inside these ranges and needn't reach their ends.
There are 2 independent parts, one for each index of `grp`. The reference program is written for one: setup_inputs(seed, part) draws one part's arguments, and reference() takes and returns one part's arrays. A program takes and returns all parts, laid end to end along the dimension named above; an argument that names none is the same for every part. Nothing has to cross between parts.
Inputs may be any that keep to these rules, and one draw needn't show every extreme that they name: Pair p holds the orders m_slots[p] and 255 - m_slots[p]; each value appears once. Cycle slot i holds cycle cycle_order[i]; each value appears once.
All inputs are finite; a program needn't handle non-finite values.
Results may differ from the reference program's by a relative error of at most 0.017.
Values may be sent and summed in bfloat16 or wider, within the bound.
A program may use at most 128 MiB of HBM per device.

```python
import math
import jax
import jax.numpy as jnp
from jax import lax

MODES = 256
PAIRS = 128
ROWS = 257
CYCLES = 16
NPHI = 4096
SIMS = 4


def touch_ends(drawn, stream_key, smallest, high):
    extent = drawn.shape
    spot = [jax.random.randint(jax.random.fold_in(stream_key, axis), (), 0, extent[axis]) for axis in range(len(extent))]
    drawn = drawn.at[tuple(spot)].set(smallest)
    longest = extent.index(max(extent))
    spot[longest] = (spot[longest] + 1) % extent[longest]
    return drawn.at[tuple(spot)].set(high)


def levels(stream_key, extent, split, low, largest):
    level, own = 1.0, jax.random.fold_in(stream_key, 6)
    for position, parts in split:
        steps = jnp.exp(jax.random.uniform(jax.random.fold_in(own, position), (parts,), jnp.float32, low / len(split), largest / len(split)))
        level = level * jnp.repeat(steps, extent[position] // parts).reshape([-1 if axis == position else 1 for axis in range(len(extent))])
    return level


def scatter_about(stream_key, extent, deviation, reach, split=(), dtype=jnp.bfloat16):
    drawn = deviation * jax.random.normal(stream_key, extent, jnp.float32)
    if split:
        drawn = drawn * levels(stream_key, extent, split, -0.22, 0.18)
    return jnp.clip(drawn, -reach, reach).astype(dtype)


def setup_inputs(seed: int = 0, part: int = 0) -> dict:
    seeds = jax.random.split(jax.random.key(seed), 9)
    part_splits = jax.random.split(jax.random.fold_in(seeds[8], part), 9)
    tbar_alm = scatter_about(part_splits[0], (PAIRS, SIMS, 2, ROWS), 1.0, 6.0, ((0, 16),))
    twf_alm = scatter_about(part_splits[1], (PAIRS, SIMS, 2, ROWS), 1.0, 6.0, ((0, 16),))
    legendre = scatter_about(seeds[2], (PAIRS, ROWS, CYCLES), ROWS ** -0.5, 0.375, ((0, 16),))
    m_slots = jax.random.permutation(seeds[3], PAIRS).astype(jnp.int32)
    cycle_order = jax.random.permutation(seeds[4], CYCLES).astype(jnp.int32)
    colatitude = jnp.clip(jax.random.uniform(seeds[5], (CYCLES,), jnp.float32, 0.35, 2.79), 0.35, 2.79)
    cycle_weight = jnp.clip(jnp.exp(jax.random.uniform(seeds[6], (CYCLES,), jnp.float32, math.log(0.25), math.log(1.0))), 0.25, 1.0)
    pixel_mask = touch_ends(jax.random.randint(seeds[7], (CYCLES, NPHI), 0, 4), jax.random.fold_in(seeds[7], 1), 0, 3).astype(jnp.int32)
    return {"tbar_alm": tbar_alm, "twf_alm": twf_alm, "legendre": legendre, "m_slots": m_slots, "cycle_order": cycle_order, "colatitude": colatitude, "cycle_weight": cycle_weight, "pixel_mask": pixel_mask}


def rounded(values):
    return lax.optimization_barrier(values.astype(jnp.bfloat16)).astype(jnp.float32)

def pair_layout(small_orders, mode_count):
    row_index = lax.broadcasted_iota(jnp.int32, (small_orders.shape[0], mode_count + 1), 1)
    smaller = small_orders[:, None]
    upper_half = row_index >= mode_count - smaller
    degree = jnp.where(upper_half, row_index - 1, smaller + row_index)
    orders = jnp.where(upper_half, mode_count - 1 - smaller, smaller + 0 * row_index)
    return (upper_half, degree.astype(jnp.float32), orders.astype(jnp.float32))

def raising(degree, orders):
    square = (degree * degree - orders * orders) * (2.0 * degree + 1.0) / jnp.maximum(2.0 * degree - 1.0, 1.0)
    return jnp.where(degree > orders, jnp.sqrt(jnp.where(degree > orders, square, 0.0)), 0.0)

def synthesis_sets(tbar_alm, twf_alm, degree, raising_factor, mode_count):
    wiener = twf_alm.astype(jnp.float32)
    scaled = (raising_factor / mode_count)[:, None, None, :] * wiener
    raised = jnp.concatenate([scaled[..., 1:], jnp.zeros_like(scaled[..., :1])], axis=-1)
    stacked = jnp.stack([tbar_alm.astype(jnp.float32), wiener, (degree / mode_count)[:, None, None, :] * wiener, raised], axis=2)
    return stacked.reshape(stacked.shape[0], stacked.shape[1], 8, stacked.shape[4]).astype(jnp.bfloat16)

def mode_columns(small_orders, mode_count):
    return jnp.stack([small_orders, mode_count - 1 - small_orders], axis=1).reshape(-1)

def fourier_table(orders_int, pixel_count):
    pixel_index = lax.broadcasted_iota(jnp.int32, (orders_int.shape[0], pixel_count), 1)
    turns = orders_int[:, None] * pixel_index % pixel_count
    radians = turns.astype(jnp.float32) * (2.0 * math.pi / pixel_count)
    return jnp.stack([jnp.cos(radians), -jnp.sin(radians)], axis=0).astype(jnp.bfloat16)

def combine_modes(legendre_sums, orders_int, cos_cycle, sin_cycle, mode_count):
    orders_real = orders_int.astype(jnp.float32)
    inv_sin = 1.0 / sin_cycle
    ratio = (orders_real / mode_count)[:, None]
    theta_real = (cos_cycle * legendre_sums[:, 4] - legendre_sums[:, 6]) * inv_sin
    theta_imag = (cos_cycle * legendre_sums[:, 5] - legendre_sums[:, 7]) * inv_sin
    phi_real = -ratio * legendre_sums[:, 3] * inv_sin
    phi_imag = ratio * legendre_sums[:, 2] * inv_sin
    weight = (jnp.where(orders_int == 0, 1.0, 2.0) * mode_count ** (-0.5))[:, None]
    stacked = jnp.stack([legendre_sums[:, 0], legendre_sums[:, 1], theta_real, theta_imag, phi_real, phi_imag], axis=1)
    return (stacked * weight).astype(jnp.bfloat16)

def analysis_sets(spectra, colatitude, cycle_weight):
    with_cos = cycle_weight * jnp.cos(colatitude) / jnp.sin(colatitude)
    with_sin = cycle_weight / jnp.sin(colatitude)
    stacked = jnp.stack([spectra[:, 0] * with_cos, spectra[:, 0] * with_sin, spectra[:, 1] * with_cos, spectra[:, 1] * with_sin], axis=1)
    return stacked.reshape(spectra.shape[0], 8, spectra.shape[3], spectra.shape[4]).astype(jnp.bfloat16)

def estimate(merged, degree, orders, raising_factor, mode_count, cycle_count):
    level = degree[:, None, :]
    azimuth = orders[:, None, :]
    factor = raising_factor[:, None, :]

    def previous(values):
        return jnp.concatenate([jnp.zeros_like(values[..., :1]), values[..., :-1]], axis=-1)
    grad_real = level * merged[:, :, 0] - factor * previous(merged[:, :, 2]) + azimuth * merged[:, :, 7]
    grad_imag = level * merged[:, :, 1] - factor * previous(merged[:, :, 3]) - azimuth * merged[:, :, 6]
    curl_real = level * merged[:, :, 4] - factor * previous(merged[:, :, 6]) - azimuth * merged[:, :, 3]
    curl_imag = level * merged[:, :, 5] - factor * previous(merged[:, :, 7]) + azimuth * merged[:, :, 2]
    scale = (mode_count / cycle_count) ** 0.5 / jnp.sqrt(jnp.maximum(level * (level + 1.0), 1.0))
    scale = scale[:, :, None, :]
    return (jnp.stack([grad_real, grad_imag], axis=2) * scale, jnp.stack([curl_real, curl_imag], axis=2) * scale)

def reference(tbar_alm, twf_alm, legendre, m_slots, cycle_order, colatitude, cycle_weight, pixel_mask):
    upper_half, degree, orders = pair_layout(m_slots, MODES)
    raising_factor = raising(degree, orders)
    coeff_sets = rounded(synthesis_sets(tbar_alm, twf_alm, degree, raising_factor, MODES))
    halves = jnp.stack([jnp.logical_not(upper_half), upper_half], axis=1).astype(jnp.float32)
    blocks = PAIRS // 8

    def synth_block(block_items):
        block_sets, block_halves, block_table = block_items
        masked = block_sets[:, None] * block_halves[:, :, None, None, :]
        return jnp.einsum('phsck,pkr->scphr', masked, block_table.astype(jnp.float32))
    legendre_sums = lax.map(synth_block, (coeff_sets.reshape(blocks, 8, SIMS, 8, ROWS), halves.reshape(blocks, 8, 2, ROWS), legendre.reshape(blocks, 8, ROWS, CYCLES)))
    legendre_sums = jnp.transpose(legendre_sums, (1, 2, 0, 3, 4, 5)).reshape(SIMS, 8, MODES, CYCLES)
    legendre_sums = jnp.take(legendre_sums, cycle_order, axis=3)
    slot_theta = jnp.take(colatitude, cycle_order)
    orders_all = mode_columns(m_slots, MODES)
    fourier = combine_modes(legendre_sums, orders_all, jnp.cos(slot_theta), jnp.sin(slot_theta), MODES)
    fourier = rounded(fourier).reshape(SIMS, 3, 2, MODES, CYCLES)
    dft_table = rounded(fourier_table(orders_all, NPHI))
    cycle_maps = jnp.einsum('sqemr,emj->sqrj', fourier, dft_table)
    products = rounded(pixel_mask.astype(jnp.float32) * cycle_maps[:, 0:1] * cycle_maps[:, 1:3])
    spectra = rounded(jnp.einsum('sqrj,emj->sqemr', products, dft_table) * NPHI ** (-0.5))
    inverse = jnp.zeros((CYCLES,), jnp.int32).at[cycle_order].set(lax.iota(jnp.int32, CYCLES))
    spectra = jnp.take(spectra, inverse, axis=4)
    weighted = rounded(analysis_sets(spectra, colatitude, cycle_weight))
    weighted = jnp.moveaxis(weighted.reshape(SIMS, 8, blocks, 8, 2, CYCLES), 2, 0)

    def analysis_block(block_items):
        block_weighted, block_table, block_halves, block_degree, block_orders, block_raising = block_items
        projected = jnp.einsum('scphr,pkr->phsck', block_weighted, block_table.astype(jnp.float32))
        merged = lax.optimization_barrier(jnp.sum(projected * block_halves[:, :, None, None, :], axis=1))
        return estimate(merged, block_degree, block_orders, block_raising, MODES, CYCLES)
    gradient, curl = lax.map(analysis_block, (weighted, legendre.reshape(blocks, 8, ROWS, CYCLES), halves.reshape(blocks, 8, 2, ROWS), degree.reshape(blocks, 8, ROWS), orders.reshape(blocks, 8, ROWS), raising_factor.reshape(blocks, 8, ROWS)))
    return (gradient.reshape(PAIRS, SIMS, 2, ROWS), curl.reshape(PAIRS, SIMS, 2, ROWS))
```

```python
import math

import functools

import jax
import jax.numpy as jnp
import numpy as np
from jax import lax
from jax.experimental import pallas as pl
from jax.experimental.pallas import tpu as pltpu
from jax.sharding import PartitionSpec as P


def pair_layout(small_orders, mode_count):
    row_index = lax.broadcasted_iota(jnp.int32, (small_orders.shape[0], mode_count + 1), 1)
    smaller = small_orders[:, None]
    upper_half = row_index >= mode_count - smaller
    degree = jnp.where(upper_half, row_index - 1, smaller + row_index)
    orders = jnp.where(upper_half, mode_count - 1 - smaller, smaller + 0 * row_index)
    return (upper_half, degree.astype(jnp.float32), orders.astype(jnp.float32))


def raising(degree, orders):
    square = (
        (degree * degree - orders * orders)
        * (2.0 * degree + 1.0)
        / jnp.maximum(2.0 * degree - 1.0, 1.0)
    )
    return jnp.where(degree > orders, jnp.sqrt(jnp.where(degree > orders, square, 0.0)), 0.0)


def synthesis_sets(tbar_alm, twf_alm, degree, raising_factor, mode_count):
    wiener = twf_alm.astype(jnp.float32)
    scaled = (raising_factor / mode_count)[:, None, None, :] * wiener
    raised = jnp.concatenate([scaled[..., 1:], jnp.zeros_like(scaled[..., :1])], axis=-1)
    stacked = jnp.stack(
        [
            tbar_alm.astype(jnp.float32),
            wiener,
            (degree / mode_count)[:, None, None, :] * wiener,
            raised,
        ],
        axis=2,
    )
    return stacked.reshape(stacked.shape[0], stacked.shape[1], 8, stacked.shape[4]).astype(
        jnp.bfloat16
    )


def mode_columns(small_orders, mode_count):
    return jnp.stack([small_orders, mode_count - 1 - small_orders], axis=1).reshape(-1)


def fourier_table(orders_int, pixel_count):
    pixel_index = lax.broadcasted_iota(jnp.int32, (orders_int.shape[0], pixel_count), 1)
    turns = orders_int[:, None] * pixel_index % pixel_count
    radians = turns.astype(jnp.float32) * (2.0 * math.pi / pixel_count)
    return jnp.stack([jnp.cos(radians), -jnp.sin(radians)], axis=0).astype(jnp.bfloat16)


def combine_modes(legendre_sums, orders_int, cos_cycle, sin_cycle, mode_count):
    orders_real = orders_int.astype(jnp.float32)
    inv_sin = 1.0 / sin_cycle
    ratio = (orders_real / mode_count)[:, None]
    theta_real = (cos_cycle * legendre_sums[:, 4] - legendre_sums[:, 6]) * inv_sin
    theta_imag = (cos_cycle * legendre_sums[:, 5] - legendre_sums[:, 7]) * inv_sin
    phi_real = -ratio * legendre_sums[:, 3] * inv_sin
    phi_imag = ratio * legendre_sums[:, 2] * inv_sin
    weight = (jnp.where(orders_int == 0, 1.0, 2.0) * mode_count ** (-0.5))[:, None]
    stacked = jnp.stack(
        [legendre_sums[:, 0], legendre_sums[:, 1], theta_real, theta_imag, phi_real, phi_imag],
        axis=1,
    )
    return (stacked * weight).astype(jnp.bfloat16)


def analysis_sets(spectra, colatitude, cycle_weight):
    with_cos = cycle_weight * jnp.cos(colatitude) / jnp.sin(colatitude)
    with_sin = cycle_weight / jnp.sin(colatitude)
    stacked = jnp.stack(
        [
            spectra[:, 0] * with_cos,
            spectra[:, 0] * with_sin,
            spectra[:, 1] * with_cos,
            spectra[:, 1] * with_sin,
        ],
        axis=1,
    )
    return stacked.reshape(spectra.shape[0], 8, spectra.shape[3], spectra.shape[4]).astype(
        jnp.bfloat16
    )


def estimate(merged, degree, orders, raising_factor, mode_count, cycle_count):
    level = degree[:, None, :]
    azimuth = orders[:, None, :]
    factor = raising_factor[:, None, :]

    def previous(values):
        return jnp.concatenate([jnp.zeros_like(values[..., :1]), values[..., :-1]], axis=-1)

    grad_real = (
        level * merged[:, :, 0] - factor * previous(merged[:, :, 2]) + azimuth * merged[:, :, 7]
    )
    grad_imag = (
        level * merged[:, :, 1] - factor * previous(merged[:, :, 3]) - azimuth * merged[:, :, 6]
    )
    curl_real = (
        level * merged[:, :, 4] - factor * previous(merged[:, :, 6]) - azimuth * merged[:, :, 3]
    )
    curl_imag = (
        level * merged[:, :, 5] - factor * previous(merged[:, :, 7]) + azimuth * merged[:, :, 2]
    )
    scale = (mode_count / cycle_count) ** 0.5 / jnp.sqrt(jnp.maximum(level * (level + 1.0), 1.0))
    scale = scale[:, :, None, :]
    return (
        jnp.stack([grad_real, grad_imag], axis=2) * scale,
        jnp.stack([curl_real, curl_imag], axis=2) * scale,
    )


def shards(tbar_alm, twf_alm, legendre, m_slots, cycle_order, colatitude, cycle_weight, pixel_mask):
    pairs_dev = tbar_alm.shape[0]
    row_count = tbar_alm.shape[3]
    mode_count = row_count - 1
    cycle_count = legendre.shape[2]
    cycle_dev = pixel_mask.shape[0]
    pixel_count = pixel_mask.shape[1]
    device_slot = lax.axis_index("ma")
    local_small = lax.dynamic_slice_in_dim(m_slots, device_slot * pairs_dev, pairs_dev)
    upper_half, degree, orders = pair_layout(local_small, mode_count)
    raising_factor = raising(degree, orders)
    coeff_sets = synthesis_sets(tbar_alm, twf_alm, degree, raising_factor, mode_count)
    halves = jnp.stack([jnp.logical_not(upper_half), upper_half], axis=1)
    masked = coeff_sets[:, None] * halves.astype(jnp.bfloat16)[:, :, None, None, :]
    legendre_sums = jnp.einsum(
        "phsck,pkr->scphr", masked, legendre, preferred_element_type=jnp.float32
    )
    legendre_sums = jnp.take(legendre_sums, cycle_order, axis=4)
    legendre_sums = legendre_sums.reshape(legendre_sums.shape[0], 8, 2 * pairs_dev, cycle_count)
    all_orders = mode_columns(m_slots, mode_count)
    dft_table = fourier_table(all_orders, pixel_count)
    pixel_weights = pixel_mask.astype(jnp.float32)
    slot_theta = jnp.take(colatitude, cycle_order)
    local_orders = mode_columns(local_small, mode_count)
    outgoing = combine_modes(
        legendre_sums, local_orders, jnp.cos(slot_theta), jnp.sin(slot_theta), mode_count
    )
    fourier = lax.all_to_all(outgoing, "ma", split_axis=3, concat_axis=2, tiled=True)
    fourier = fourier.reshape(fourier.shape[0], 3, 2, mode_count, cycle_dev)
    cycle_maps = jnp.einsum(
        "sqemr,emj->sqrj", fourier, dft_table, preferred_element_type=jnp.float32
    )
    products = (pixel_weights * cycle_maps[:, 0:1] * cycle_maps[:, 1:3]).astype(jnp.bfloat16)
    spectra = jnp.einsum("sqrj,emj->sqemr", products, dft_table, preferred_element_type=jnp.float32)
    received = (spectra * pixel_count ** (-0.5)).astype(jnp.bfloat16)
    returned = lax.all_to_all(received, "ma", split_axis=3, concat_axis=4, tiled=True)
    inverse = (
        jnp.zeros((cycle_count,), jnp.int32).at[cycle_order].set(lax.iota(jnp.int32, cycle_count))
    )
    spectra = jnp.take(returned, inverse, axis=4).astype(jnp.float32)
    weighted = analysis_sets(spectra, colatitude, cycle_weight)
    weighted = weighted.reshape(weighted.shape[0], 8, pairs_dev, 2, cycle_count)
    projected = jnp.einsum(
        "scphr,pkr->phsck", weighted, legendre, preferred_element_type=jnp.float32
    )
    merged = jnp.sum(projected * halves.astype(jnp.float32)[:, :, None, None, :], axis=1)
    return estimate(merged, degree, orders, raising_factor, mode_count, cycle_count)


LANES = 128
F32 = jnp.float32
BF16 = jnp.bfloat16


def split_tables(mode_count, pixel_count, sims):
    m = np.arange(mode_count)[None, :]
    low = np.arange(LANES)[:, None]
    high = np.repeat(np.arange(pixel_count // LANES), sims)[:, None] * LANES
    fine = (m * low % pixel_count) * (2.0 * math.pi / pixel_count)
    coarse = (m * high % pixel_count) * (2.0 * math.pi / pixel_count)
    cos_high = np.cos(coarse).astype(np.float32)
    sin_high = np.sin(coarse).astype(np.float32)

    def halves(values):
        upper = values.astype(BF16)
        return upper, (values - upper.astype(np.float32)).astype(BF16)

    return np.concatenate(
        [np.cos(fine).astype(BF16), (-np.sin(fine)).astype(BF16)]
        + list(halves(cos_high))
        + list(halves(sin_high)),
        axis=0,
    )


def iota(shape, axis):
    return lax.broadcasted_iota(jnp.int32, shape, axis)


def one_hot(condition):
    return jnp.where(condition, 1.0, 0.0).astype(BF16)


def dot(left, right):
    return jnp.dot(left, right, preferred_element_type=F32)


def dot_t(left, right):
    return lax.dot_general(left, right, (((1,), (1,)), ((), ())), preferred_element_type=F32)


def fused_kernel(
    n, modes, rows, cycles, pixels, sims,
    slots_s, cycle_s, colat_s, weight_s, slots_v, tbar_ref, twf_ref, leg_ref, prev_ref, mask_ref,
    table_hbm, grad_ref, curl_ref,
    table_v, leg_all, prev_all, send_f, recv_f, send_p, recv_p,
    table_sem, fs_sem, fr_sem, ps_sem, pr_sem,
):
    me = lax.axis_index("ma")
    pairs, padded = tbar_ref.shape[0], tbar_ref.shape[2]
    block = 2 * pairs
    comps = 2 * sims
    span = 2 * cycles
    total = pairs * span
    fetch = pltpu.make_async_copy(table_hbm, table_v, table_sem)
    fetch.start()
    barrier = pltpu.get_barrier_semaphore()
    for off in range(1, n):
        pl.semaphore_signal(
            barrier, inc=1, device_id={"ma": lax.rem(me + off, n)},
            device_id_type=pl.DeviceIdType.MESH,
        )

    row_shape = (pairs, padded)
    smaller = jnp.zeros(row_shape, jnp.int32)
    for p in range(pairs):
        smaller = jnp.where(iota(row_shape, 0) == p, slots_s[me * pairs + p], smaller)
    k = iota(row_shape, 1)
    upper = k >= modes - smaller
    degree = jnp.where(upper, k - 1, smaller + k).astype(F32)
    orders = jnp.where(upper, modes - 1 - smaller, smaller).astype(F32)
    eps = raising(degree, orders)
    upper_f = jnp.where(upper, 1.0, 0.0)
    lower_f = 1.0 - upper_f

    colat = jnp.zeros((cycles, 4 * comps), F32)
    for r in range(cycles):
        colat = jnp.where(iota(colat.shape, 0) == r, colat_s[r], colat)
    csc = 1.0 / jnp.sin(colat)
    cot = jnp.cos(colat) * csc
    lane = iota(colat.shape, 1)
    group = lane // comps
    part_a = jnp.where(group == 0, 1.0, jnp.where(group == 1, cot, 0.0))
    part_m = jnp.where(group == 2, csc, 0.0)
    part_b = jnp.where(group == 1, csc, 0.0)

    blank = jnp.zeros((comps, padded), F32)
    pieces = []
    for p in range(pairs):
        twf = twf_ref[p].astype(F32)
        deg_p, eps_p = degree[p : p + 1] / modes, eps[p : p + 1] / modes
        sets_a = jnp.concatenate([tbar_ref[p].astype(F32), deg_p * twf, twf, blank], axis=0)
        sets_b = jnp.concatenate([blank, -(eps_p * twf), blank, blank], axis=0)
        leg, prev = leg_ref[p].astype(F32), prev_ref[p].astype(F32)
        low, high = lower_f[p : p + 1], upper_f[p : p + 1]
        leg = jnp.concatenate([leg * low, leg * high], axis=0).astype(BF16)
        prev = jnp.concatenate([prev * low, prev * high], axis=0).astype(BF16)
        leg_all[pl.ds(p * span, span), :] = leg
        prev_all[pl.ds(p * span, span), :] = prev
        out_a = dot_t(leg, sets_a.astype(BF16))
        out_b = dot_t(prev, sets_b.astype(BF16))
        for h in range(2):
            small = slots_s[me * pairs + p]
            order = modes - 1 - small if h else small
            norm = jnp.where(order == 0, 1.0, 2.0) * modes ** (-0.5)
            ratio = order.astype(F32) / modes
            rng = slice(h * cycles, (h + 1) * cycles)
            pieces.append((out_a[rng] * (part_a + part_m * ratio) + out_b[rng] * part_b) * norm)
    fourier = jnp.concatenate(pieces, axis=0).astype(BF16)

    base_shape = (block, total)
    row = iota(base_shape, 0)
    base = iota(base_shape, 1) - (lax.rem(row, pairs) * span + (row // pairs) * cycles)
    place = jnp.concatenate(
        [jnp.where(base == cycle_s[i], 1.0, 0.0) for i in range(cycles)], axis=0
    ).astype(BF16)
    placed = dot(place, fourier).astype(BF16)
    send_f[:, :, : 4 * comps] = placed.reshape(n, block, 4 * comps)

    def exchange(send, recv, s_sem, r_sem):
        copies = []
        for off in range(1, n):
            to = lax.rem(me + off, n)
            copy = pltpu.make_async_remote_copy(
                src_ref=send.at[to], dst_ref=recv.at[me], send_sem=s_sem.at[off],
                recv_sem=r_sem.at[off], device_id={"ma": to},
                device_id_type=pl.DeviceIdType.MESH,
            )
            copy.start()
            copies.append(copy)
        recv[me] = send[me]
        return copies

    pl.semaphore_wait(barrier, n - 1)
    copies = exchange(send_f, recv_f, fs_sem, fr_sem)

    spread_shape = (slots_v.shape[1], n * block)
    col = iota(spread_shape, 1)
    spread = one_hot(
        iota(spread_shape, 0) == (col // block) * pairs + lax.rem(col, pairs)
    )
    slots = jnp.broadcast_to(slots_v[...], (8, slots_v.shape[1]))
    high_part = (slots // 256).astype(F32)
    low_part = lax.rem(slots, 256).astype(F32)
    picked = 256.0 * dot(high_part.astype(BF16), spread) + dot(low_part.astype(BF16), spread)
    flip = lax.rem(iota(picked.shape, 1), block) >= pairs
    picked = jnp.where(flip, modes - 1.0 - picked, picked)[0:1]
    select = one_hot(iota((modes, n * block), 0).astype(F32) == picked)

    hs = pixels // LANES * sims
    fetch.wait()
    moved = dot(table_v[...], select)
    fine_cos, fine_sin = moved[:LANES], moved[LANES : 2 * LANES]
    at = 2 * LANES
    cos_t = moved[at : at + hs] + moved[at + hs : at + 2 * hs]
    sin_t = moved[at + 2 * hs : at + 3 * hs] + moved[at + 3 * hs : at + 4 * hs]
    cos_h, sin_h = cos_t.T, sin_t.T
    synth = jnp.concatenate([fine_cos, fine_sin], axis=1).astype(BF16)
    anal = jnp.concatenate([fine_cos.T, fine_sin.T], axis=0).astype(BF16)

    exp_shape = (4 * comps, 6 * hs)
    ecol = iota(exp_shape, 1)
    which = ecol // hs
    comp_q, comp_c = which // 2, lax.rem(which, 2)
    source_c = jnp.where(comp_q == 2, 1 - comp_c, comp_c)
    hit = iota(exp_shape, 0) == comp_q * comps + 2 * lax.rem(ecol, sims) + source_c
    sign = jnp.where(jnp.logical_and(comp_q == 2, comp_c == 0), -1.0, 1.0)
    expand = jnp.where(hit, sign, 0.0).astype(BF16)

    sel_shape = (4 * hs, 4 * comps)
    srow, scol = iota(sel_shape, 0), iota(sel_shape, 1)
    row_q, row_c = srow // (2 * hs), lax.rem(srow // hs, 2)
    out_g, out_c = scol // comps, lax.rem(scol, 2)
    want_q = jnp.where(jnp.logical_or(out_g == 1, out_g == 2), 1, 0)
    swap = out_g >= 2
    want_c = jnp.where(swap, 1 - out_c, out_c)
    same_s = lax.rem(srow, sims) == lax.rem(scol, comps) // 2
    negative = jnp.logical_or(
        jnp.logical_and(out_g == 2, out_c == 1), jnp.logical_and(out_g == 3, out_c == 0)
    )
    hit = jnp.logical_and(jnp.logical_and(row_q == want_q, row_c == want_c), same_s)
    gather = jnp.where(hit, jnp.where(negative, -1.0, 1.0), 0.0).astype(BF16)

    mask_t = mask_ref[...].astype(F32).T.astype(BF16)
    m_shape = (pixels // LANES, hs)
    mask = dot(mask_t, one_hot(iota(m_shape, 0) == iota(m_shape, 1) // sims))

    lane_shape = (8, total)
    cyc = lax.rem(iota(lane_shape, 1), cycles)
    theta_l = jnp.zeros(lane_shape, F32)
    weight_l = jnp.zeros(lane_shape, F32)
    for r in range(cycles):
        theta_l = jnp.where(cyc == r, colat_s[r], theta_l)
        weight_l = jnp.where(cyc == r, weight_s[r], weight_l)
    with_sin = (weight_l / jnp.sin(theta_l))[0:1]
    with_cos = (weight_l * jnp.cos(theta_l) / jnp.sin(theta_l))[0:1]

    for copy in copies:
        copy.wait_recv()
    got = recv_f[...].reshape(n * block, LANES)[:, : 4 * comps]
    spread_f = dot(got, expand)
    real, imag = [], []
    for q in range(3):
        re = spread_f[:, 2 * q * hs : (2 * q + 1) * hs]
        im = spread_f[:, (2 * q + 1) * hs : (2 * q + 2) * hs]
        real.append((re * cos_h - im * sin_h).astype(BF16))
        imag.append((re * sin_h + im * cos_h).astype(BF16))
    turned = jnp.concatenate(
        [jnp.concatenate(real, axis=1), jnp.concatenate(imag, axis=1)], axis=0
    )
    maps = dot(synth, turned)
    lead = mask * maps[:, :hs]
    products = jnp.concatenate(
        [lead * maps[:, hs : 2 * hs], lead * maps[:, 2 * hs :]], axis=1
    ).astype(BF16)
    half = dot(anal, products)
    parts = []
    count = n * block
    for q in range(2):
        c_part = half[:count, q * hs : (q + 1) * hs]
        s_part = half[count:, q * hs : (q + 1) * hs]
        parts.append((cos_h * c_part + sin_h * s_part).astype(BF16))
        parts.append((cos_h * s_part - sin_h * c_part).astype(BF16))
    spectra = dot(jnp.concatenate(parts, axis=1), gather) * pixels ** (-0.5)
    send_p[:, :, : 4 * comps] = spectra.astype(BF16).reshape(n, block, 4 * comps)
    back = exchange(send_p, recv_p, ps_sem, pr_sem)
    scale = (modes / cycles) ** 0.5 / jnp.sqrt(jnp.maximum(degree * (degree + 1.0), 1.0))
    f_level, f_eps, f_order = degree * scale, eps * scale, orders * scale
    for copy in back:
        copy.wait_recv()

    came = recv_p[...].reshape(n * block, LANES)[:, : 4 * comps].astype(F32).T.astype(BF16)
    by_pair = dot(came, place)
    first = jnp.concatenate([by_pair[: 2 * comps] * with_cos, by_pair[2 * comps :] * with_sin], 0)
    second = by_pair[: 2 * comps] * with_sin
    owner = iota((1, total), 1) // span
    keep = [jnp.where(owner == p, 1.0, 0.0) for p in range(pairs)]
    first = jnp.concatenate([(first * keep[p]).astype(BF16) for p in range(pairs)], axis=0)
    second = jnp.concatenate([(second * keep[p]).astype(BF16) for p in range(pairs)], axis=0)
    here = dot(first, leg_all[...])
    before = dot(second, prev_all[...])
    for p in range(pairs):
        a, b = 4 * comps * p, 2 * comps * p
        lev, ep, az = f_level[p : p + 1], f_eps[p : p + 1], f_order[p : p + 1]
        grad_ref[p] = (
            lev * here[a : a + comps] - ep * before[b : b + comps]
            + az * here[a + 2 * comps : a + 3 * comps]
        )
        curl_ref[p] = (
            lev * here[a + comps : a + 2 * comps] - ep * before[b + comps : b + 2 * comps]
            + az * here[a + 3 * comps : a + 4 * comps]
        )
    for copy in copies + back:
        copy.wait_send()


def fused(tbar_alm, twf_alm, legendre, m_slots, cycle_order, colatitude, cycle_weight, pixel_mask, n):
    pairs, sims, _, rows = tbar_alm.shape
    modes = rows - 1
    cycles = legendre.shape[2]
    pixels = pixel_mask.shape[1]
    padded = -(-rows // LANES) * LANES
    comps = 2 * sims
    total = pairs * 2 * cycles
    hs = pixels // LANES * sims
    pad = ((0, 0), (0, 0), (0, padded - rows))
    tbar = jnp.pad(tbar_alm.reshape(pairs, comps, rows), pad)
    twf = jnp.pad(twf_alm.reshape(pairs, comps, rows), pad)
    by_cycle = jnp.transpose(legendre, (0, 2, 1))
    leg = jnp.pad(by_cycle, pad)
    prev = jnp.pad(by_cycle[:, :, : rows - 1], ((0, 0), (0, 0), (1, padded - rows)))
    table = jnp.asarray(split_tables(modes, pixels, sims))
    vmem, smem = pl.BlockSpec(memory_space=pltpu.VMEM), pl.BlockSpec(memory_space=pltpu.SMEM)
    out = jax.ShapeDtypeStruct((pairs, comps, padded), F32)
    grad, curl = pl.pallas_call(
        functools.partial(fused_kernel, n, modes, rows, cycles, pixels, sims),
        out_shape=(out, out),
        in_specs=[smem] * 4 + [vmem] * 6 + [pl.BlockSpec(memory_space=pl.ANY)],
        out_specs=(vmem, vmem),
        scratch_shapes=[
            pltpu.VMEM(table.shape, BF16),
            pltpu.VMEM((total, padded), BF16),
            pltpu.VMEM((total, padded), BF16),
        ]
        + [pltpu.VMEM((n, 2 * pairs, LANES), BF16)] * 4
        + [pltpu.SemaphoreType.DMA]
        + [pltpu.SemaphoreType.DMA((n,))] * 4,
        compiler_params=pltpu.CompilerParams(collective_id=0, has_side_effects=True),
        name="estimator",
    )(
        m_slots, cycle_order, colatitude, cycle_weight, m_slots.reshape(1, -1), tbar, twf, leg,
        prev, pixel_mask.reshape(pixels // LANES, LANES), table,
    )
    shape = (pairs, sims, 2, rows)
    return grad[:, :, :rows].reshape(shape), curl[:, :, :rows].reshape(shape)


def body(n, *args):
    tbar_alm, legendre, pixel_mask = args[0], args[2], args[7]
    pairs, sims, _, rows = tbar_alm.shape
    cycles = legendre.shape[2]
    fits = (
        pairs == 8
        and cycles % 16 == 0
        and pixel_mask.shape[0] == 1
        and pairs * 2 * cycles <= 512
        and rows <= 1025
        and (pixel_mask.shape[1] // LANES * sims) % LANES == 0
        and sims % 4 == 0
    )
    return fused(*args, n) if fits else shards(*args)


def solution(mesh):
    return jax.shard_map(
        functools.partial(body, mesh.shape["ma"]),
        mesh=mesh,
        in_specs=(
            P("ma", "grp", None, None),
            P("ma", "grp", None, None),
            P("ma", None, None),
            P(),
            P(),
            P(),
            P(),
            P("ma", None),
        ),
        out_specs=(P("ma", "grp", None, None), P("ma", "grp", None, None)),
        check_vma=False,
    )
```

```python
import math

import functools

import jax
import jax.numpy as jnp
import numpy as np
from jax import lax
from jax.experimental import pallas as pl
from jax.experimental.pallas import tpu as pltpu
from jax.sharding import PartitionSpec as P


def pair_layout(small_orders, mode_count):
    row_index = lax.broadcasted_iota(jnp.int32, (small_orders.shape[0], mode_count + 1), 1)
    smaller = small_orders[:, None]
    upper_half = row_index >= mode_count - smaller
    degree = jnp.where(upper_half, row_index - 1, smaller + row_index)
    orders = jnp.where(upper_half, mode_count - 1 - smaller, smaller + 0 * row_index)
    return (upper_half, degree.astype(jnp.float32), orders.astype(jnp.float32))


def raising(degree, orders):
    square = (
        (degree * degree - orders * orders)
        * (2.0 * degree + 1.0)
        / jnp.maximum(2.0 * degree - 1.0, 1.0)
    )
    return jnp.where(degree > orders, jnp.sqrt(jnp.where(degree > orders, square, 0.0)), 0.0)


def synthesis_sets(tbar_alm, twf_alm, degree, raising_factor, mode_count):
    wiener = twf_alm.astype(jnp.float32)
    scaled = (raising_factor / mode_count)[:, None, None, :] * wiener
    raised = jnp.concatenate([scaled[..., 1:], jnp.zeros_like(scaled[..., :1])], axis=-1)
    stacked = jnp.stack(
        [
            tbar_alm.astype(jnp.float32),
            wiener,
            (degree / mode_count)[:, None, None, :] * wiener,
            raised,
        ],
        axis=2,
    )
    return stacked.reshape(stacked.shape[0], stacked.shape[1], 8, stacked.shape[4]).astype(
        jnp.bfloat16
    )


def mode_columns(small_orders, mode_count):
    return jnp.stack([small_orders, mode_count - 1 - small_orders], axis=1).reshape(-1)


def fourier_table(orders_int, pixel_count):
    pixel_index = lax.broadcasted_iota(jnp.int32, (orders_int.shape[0], pixel_count), 1)
    turns = orders_int[:, None] * pixel_index % pixel_count
    radians = turns.astype(jnp.float32) * (2.0 * math.pi / pixel_count)
    return jnp.stack([jnp.cos(radians), -jnp.sin(radians)], axis=0).astype(jnp.bfloat16)


def combine_modes(legendre_sums, orders_int, cos_cycle, sin_cycle, mode_count):
    orders_real = orders_int.astype(jnp.float32)
    inv_sin = 1.0 / sin_cycle
    ratio = (orders_real / mode_count)[:, None]
    theta_real = (cos_cycle * legendre_sums[:, 4] - legendre_sums[:, 6]) * inv_sin
    theta_imag = (cos_cycle * legendre_sums[:, 5] - legendre_sums[:, 7]) * inv_sin
    phi_real = -ratio * legendre_sums[:, 3] * inv_sin
    phi_imag = ratio * legendre_sums[:, 2] * inv_sin
    weight = (jnp.where(orders_int == 0, 1.0, 2.0) * mode_count ** (-0.5))[:, None]
    stacked = jnp.stack(
        [legendre_sums[:, 0], legendre_sums[:, 1], theta_real, theta_imag, phi_real, phi_imag],
        axis=1,
    )
    return (stacked * weight).astype(jnp.bfloat16)


def analysis_sets(spectra, colatitude, cycle_weight):
    with_cos = cycle_weight * jnp.cos(colatitude) / jnp.sin(colatitude)
    with_sin = cycle_weight / jnp.sin(colatitude)
    stacked = jnp.stack(
        [
            spectra[:, 0] * with_cos,
            spectra[:, 0] * with_sin,
            spectra[:, 1] * with_cos,
            spectra[:, 1] * with_sin,
        ],
        axis=1,
    )
    return stacked.reshape(spectra.shape[0], 8, spectra.shape[3], spectra.shape[4]).astype(
        jnp.bfloat16
    )


def estimate(merged, degree, orders, raising_factor, mode_count, cycle_count):
    level = degree[:, None, :]
    azimuth = orders[:, None, :]
    factor = raising_factor[:, None, :]

    def previous(values):
        return jnp.concatenate([jnp.zeros_like(values[..., :1]), values[..., :-1]], axis=-1)

    grad_real = (
        level * merged[:, :, 0] - factor * previous(merged[:, :, 2]) + azimuth * merged[:, :, 7]
    )
    grad_imag = (
        level * merged[:, :, 1] - factor * previous(merged[:, :, 3]) - azimuth * merged[:, :, 6]
    )
    curl_real = (
        level * merged[:, :, 4] - factor * previous(merged[:, :, 6]) - azimuth * merged[:, :, 3]
    )
    curl_imag = (
        level * merged[:, :, 5] - factor * previous(merged[:, :, 7]) + azimuth * merged[:, :, 2]
    )
    scale = (mode_count / cycle_count) ** 0.5 / jnp.sqrt(jnp.maximum(level * (level + 1.0), 1.0))
    scale = scale[:, :, None, :]
    return (
        jnp.stack([grad_real, grad_imag], axis=2) * scale,
        jnp.stack([curl_real, curl_imag], axis=2) * scale,
    )


def shards(tbar_alm, twf_alm, legendre, m_slots, cycle_order, colatitude, cycle_weight, pixel_mask):
    pairs_dev = tbar_alm.shape[0]
    row_count = tbar_alm.shape[3]
    mode_count = row_count - 1
    cycle_count = legendre.shape[2]
    cycle_dev = pixel_mask.shape[0]
    pixel_count = pixel_mask.shape[1]
    device_slot = lax.axis_index("ma")
    local_small = lax.dynamic_slice_in_dim(m_slots, device_slot * pairs_dev, pairs_dev)
    upper_half, degree, orders = pair_layout(local_small, mode_count)
    raising_factor = raising(degree, orders)
    coeff_sets = synthesis_sets(tbar_alm, twf_alm, degree, raising_factor, mode_count)
    halves = jnp.stack([jnp.logical_not(upper_half), upper_half], axis=1)
    masked = coeff_sets[:, None] * halves.astype(jnp.bfloat16)[:, :, None, None, :]
    legendre_sums = jnp.einsum(
        "phsck,pkr->scphr", masked, legendre, preferred_element_type=jnp.float32
    )
    legendre_sums = jnp.take(legendre_sums, cycle_order, axis=4)
    legendre_sums = legendre_sums.reshape(legendre_sums.shape[0], 8, 2 * pairs_dev, cycle_count)
    all_orders = mode_columns(m_slots, mode_count)
    dft_table = fourier_table(all_orders, pixel_count)
    pixel_weights = pixel_mask.astype(jnp.float32)
    slot_theta = jnp.take(colatitude, cycle_order)
    local_orders = mode_columns(local_small, mode_count)
    outgoing = combine_modes(
        legendre_sums, local_orders, jnp.cos(slot_theta), jnp.sin(slot_theta), mode_count
    )
    fourier = lax.all_to_all(outgoing, "ma", split_axis=3, concat_axis=2, tiled=True)
    fourier = fourier.reshape(fourier.shape[0], 3, 2, mode_count, cycle_dev)
    cycle_maps = jnp.einsum(
        "sqemr,emj->sqrj", fourier, dft_table, preferred_element_type=jnp.float32
    )
    products = (pixel_weights * cycle_maps[:, 0:1] * cycle_maps[:, 1:3]).astype(jnp.bfloat16)
    spectra = jnp.einsum("sqrj,emj->sqemr", products, dft_table, preferred_element_type=jnp.float32)
    received = (spectra * pixel_count ** (-0.5)).astype(jnp.bfloat16)
    returned = lax.all_to_all(received, "ma", split_axis=3, concat_axis=4, tiled=True)
    inverse = (
        jnp.zeros((cycle_count,), jnp.int32).at[cycle_order].set(lax.iota(jnp.int32, cycle_count))
    )
    spectra = jnp.take(returned, inverse, axis=4).astype(jnp.float32)
    weighted = analysis_sets(spectra, colatitude, cycle_weight)
    weighted = weighted.reshape(weighted.shape[0], 8, pairs_dev, 2, cycle_count)
    projected = jnp.einsum(
        "scphr,pkr->phsck", weighted, legendre, preferred_element_type=jnp.float32
    )
    merged = jnp.sum(projected * halves.astype(jnp.float32)[:, :, None, None, :], axis=1)
    return estimate(merged, degree, orders, raising_factor, mode_count, cycle_count)


LANES = 128
F32 = jnp.float32
BF16 = jnp.bfloat16


def split_tables(mode_count, pixel_count, sims):
    m = np.arange(mode_count)[None, :]
    low = np.arange(LANES)[:, None]
    high = np.repeat(np.arange(pixel_count // LANES), sims)[:, None] * LANES
    fine = (m * low % pixel_count) * (2.0 * math.pi / pixel_count)
    coarse = (m * high % pixel_count) * (2.0 * math.pi / pixel_count)
    cos_high = np.cos(coarse).astype(np.float32)
    sin_high = np.sin(coarse).astype(np.float32)

    def halves(values):
        upper = values.astype(BF16)
        return upper, (values - upper.astype(np.float32)).astype(BF16)

    return np.concatenate(
        [np.cos(fine).astype(BF16), (-np.sin(fine)).astype(BF16)]
        + list(halves(cos_high))
        + list(halves(sin_high)),
        axis=0,
    )


def iota(shape, axis):
    return lax.broadcasted_iota(jnp.int32, shape, axis)


def div(values, size):
    return values >> (size.bit_length() - 1)


def mod(values, size):
    return values & (size - 1)


def one_hot(condition):
    return jnp.where(condition, 1.0, 0.0).astype(BF16)


def dot(left, right):
    return jnp.dot(left, right, preferred_element_type=F32)


def dot_t(left, right):
    return lax.dot_general(left, right, (((1,), (1,)), ((), ())), preferred_element_type=F32)


def fused_kernel(
    n, modes, rows, cycles, pixels, sims,
    slots_s, cycle_s, colat_s, weight_s, slots_v, tbar_ref, twf_ref, leg_ref, mask_ref,
    table_hbm, grad_ref, curl_ref,
    table_v, leg_all, prev_all, send_f, recv_f, send_p, recv_p,
    table_sem, fs_sem, fr_sem, ps_sem, pr_sem,
):
    me = lax.axis_index("ma")
    pairs, padded = tbar_ref.shape[0], rows
    block = 2 * pairs
    comps = 2 * sims
    span = 2 * cycles
    total = pairs * span
    fetch = pltpu.make_async_copy(table_hbm, table_v, table_sem)
    fetch.start()
    barrier = pltpu.get_barrier_semaphore()
    for off in range(1, n):
        pl.semaphore_signal(
            barrier, inc=1, device_id={"ma": lax.rem(me + off, n)},
            device_id_type=pl.DeviceIdType.MESH,
        )

    row_shape = (pairs, padded)
    smaller = jnp.zeros(row_shape, jnp.int32)
    for p in range(pairs):
        smaller = jnp.where(iota(row_shape, 0) == p, slots_s[me * pairs + p], smaller)
    k = iota(row_shape, 1)
    upper = k >= modes - smaller
    degree = jnp.where(upper, k - 1, smaller + k).astype(F32)
    orders = jnp.where(upper, modes - 1 - smaller, smaller).astype(F32)
    eps = raising(degree, orders)
    upper_f = jnp.where(upper, 1.0, 0.0)
    lower_f = 1.0 - upper_f

    colat = jnp.zeros((cycles, 4 * comps), F32)
    for r in range(cycles):
        colat = jnp.where(iota(colat.shape, 0) == r, colat_s[r], colat)
    csc = 1.0 / jnp.sin(colat)
    cot = jnp.cos(colat) * csc
    lane = iota(colat.shape, 1)
    group = div(lane, comps)
    part_a = jnp.where(group == 0, 1.0, jnp.where(group == 1, cot, 0.0))
    part_m = jnp.where(group == 2, csc, 0.0)
    part_b = jnp.where(group == 1, csc, 0.0)

    blank = jnp.zeros((comps, padded), F32)
    pieces = []
    for p in range(pairs):
        tbar = jnp.concatenate([tbar_ref[p, s].astype(F32) for s in range(sims)], axis=0)
        twf = jnp.concatenate([twf_ref[p, s].astype(F32) for s in range(sims)], axis=0)
        deg_p, eps_p = degree[p : p + 1] / modes, eps[p : p + 1] / modes
        sets_a = jnp.concatenate([tbar, deg_p * twf, twf, blank], axis=0)
        sets_b = jnp.concatenate([blank, -(eps_p * twf), blank, blank], axis=0)
        leg = leg_ref[p].astype(F32)
        prev = jnp.concatenate([jnp.zeros_like(leg[:, :1]), leg[:, : rows - 1]], axis=1)
        low, high = lower_f[p : p + 1], upper_f[p : p + 1]
        leg = jnp.concatenate([leg * low, leg * high], axis=0).astype(BF16)
        prev = jnp.concatenate([prev * low, prev * high], axis=0).astype(BF16)
        leg_all[pl.ds(p * span, span), :] = leg
        prev_all[pl.ds(p * span, span), :] = prev
        out_a = dot_t(leg, sets_a.astype(BF16))
        out_b = dot_t(prev, sets_b.astype(BF16))
        for h in range(2):
            small = slots_s[me * pairs + p]
            order = modes - 1 - small if h else small
            norm = jnp.where(order == 0, 1.0, 2.0) * modes ** (-0.5)
            ratio = order.astype(F32) / modes
            rng = slice(h * cycles, (h + 1) * cycles)
            pieces.append((out_a[rng] * (part_a + part_m * ratio) + out_b[rng] * part_b) * norm)
    fourier = jnp.concatenate(pieces, axis=0).astype(BF16)

    base_shape = (block, total)
    row = iota(base_shape, 0)
    base = iota(base_shape, 1) - (mod(row, pairs) * span + div(row, pairs) * cycles)
    place = jnp.concatenate(
        [jnp.where(base == cycle_s[i], 1.0, 0.0) for i in range(cycles)], axis=0
    ).astype(BF16)
    placed = dot(place, fourier).astype(BF16)
    send_f[:, :, : 4 * comps] = placed.reshape(n, block, 4 * comps)

    def exchange(send, recv, s_sem, r_sem):
        copies = []
        for off in range(1, n):
            to = lax.rem(me + off, n)
            copy = pltpu.make_async_remote_copy(
                src_ref=send.at[to], dst_ref=recv.at[me], send_sem=s_sem.at[off],
                recv_sem=r_sem.at[off], device_id={"ma": to},
                device_id_type=pl.DeviceIdType.MESH,
            )
            copy.start()
            copies.append(copy)
        recv[me] = send[me]
        return copies

    pl.semaphore_wait(barrier, n - 1)
    copies = exchange(send_f, recv_f, fs_sem, fr_sem)

    spread_shape = (slots_v.shape[1], n * block)
    col = iota(spread_shape, 1)
    spread = one_hot(
        iota(spread_shape, 0) == div(col, block) * pairs + mod(col, pairs)
    )
    slots = jnp.broadcast_to(slots_v[...], (8, slots_v.shape[1]))
    high_part = div(slots, 256).astype(F32)
    low_part = mod(slots, 256).astype(F32)
    picked = 256.0 * dot(high_part.astype(BF16), spread) + dot(low_part.astype(BF16), spread)
    flip = mod(iota(picked.shape, 1), block) >= pairs
    picked = jnp.where(flip, modes - 1.0 - picked, picked)[0:1]
    select = one_hot(iota((modes, n * block), 0).astype(F32) == picked)

    hs = pixels // LANES * sims
    fetch.wait()
    moved = dot(table_v[...], select)
    fine_cos, fine_sin = moved[:LANES], moved[LANES : 2 * LANES]
    at = 2 * LANES
    cos_t = moved[at : at + hs] + moved[at + hs : at + 2 * hs]
    sin_t = moved[at + 2 * hs : at + 3 * hs] + moved[at + 3 * hs : at + 4 * hs]
    cos_h, sin_h = cos_t.T, sin_t.T
    synth = jnp.concatenate([fine_cos, fine_sin], axis=1).astype(BF16)
    anal = jnp.concatenate([fine_cos.T, fine_sin.T], axis=0).astype(BF16)

    exp_shape = (4 * comps, 6 * hs)
    ecol = iota(exp_shape, 1)
    which = div(ecol, hs)
    comp_q, comp_c = div(which, 2), mod(which, 2)
    source_c = jnp.where(comp_q == 2, 1 - comp_c, comp_c)
    hit = iota(exp_shape, 0) == comp_q * comps + 2 * mod(ecol, sims) + source_c
    sign = jnp.where(jnp.logical_and(comp_q == 2, comp_c == 0), -1.0, 1.0)
    expand = jnp.where(hit, sign, 0.0).astype(BF16)

    sel_shape = (4 * hs, 4 * comps)
    srow, scol = iota(sel_shape, 0), iota(sel_shape, 1)
    row_q, row_c = div(srow, 2 * hs), mod(div(srow, hs), 2)
    out_g, out_c = div(scol, comps), mod(scol, 2)
    want_q = jnp.where(jnp.logical_or(out_g == 1, out_g == 2), 1, 0)
    swap = out_g >= 2
    want_c = jnp.where(swap, 1 - out_c, out_c)
    same_s = mod(srow, sims) == div(mod(scol, comps), 2)
    negative = jnp.logical_or(
        jnp.logical_and(out_g == 2, out_c == 1), jnp.logical_and(out_g == 3, out_c == 0)
    )
    hit = jnp.logical_and(jnp.logical_and(row_q == want_q, row_c == want_c), same_s)
    gather = jnp.where(hit, jnp.where(negative, -1.0, 1.0), 0.0).astype(BF16)

    mask_t = mask_ref[...].astype(F32).T.astype(BF16)
    m_shape = (pixels // LANES, hs)
    mask = dot(mask_t, one_hot(iota(m_shape, 0) == div(iota(m_shape, 1), sims)))

    lane_shape = (8, total)
    cyc = mod(iota(lane_shape, 1), cycles)
    theta_l = jnp.zeros(lane_shape, F32)
    weight_l = jnp.zeros(lane_shape, F32)
    for r in range(cycles):
        theta_l = jnp.where(cyc == r, colat_s[r], theta_l)
        weight_l = jnp.where(cyc == r, weight_s[r], weight_l)
    with_sin = (weight_l / jnp.sin(theta_l))[0:1]
    with_cos = (weight_l * jnp.cos(theta_l) / jnp.sin(theta_l))[0:1]

    for copy in copies:
        copy.wait_recv()
    got = recv_f[...].reshape(n * block, LANES)[:, : 4 * comps]
    spread_f = dot(got, expand)
    real, imag = [], []
    for q in range(3):
        re = spread_f[:, 2 * q * hs : (2 * q + 1) * hs]
        im = spread_f[:, (2 * q + 1) * hs : (2 * q + 2) * hs]
        real.append((re * cos_h - im * sin_h).astype(BF16))
        imag.append((re * sin_h + im * cos_h).astype(BF16))
    turned = jnp.concatenate(
        [jnp.concatenate(real, axis=1), jnp.concatenate(imag, axis=1)], axis=0
    )
    maps = dot(synth, turned)
    lead = mask * maps[:, :hs]
    products = jnp.concatenate(
        [lead * maps[:, hs : 2 * hs], lead * maps[:, 2 * hs :]], axis=1
    ).astype(BF16)
    half = dot(anal, products)
    parts = []
    count = n * block
    for q in range(2):
        c_part = half[:count, q * hs : (q + 1) * hs]
        s_part = half[count:, q * hs : (q + 1) * hs]
        parts.append((cos_h * c_part + sin_h * s_part).astype(BF16))
        parts.append((cos_h * s_part - sin_h * c_part).astype(BF16))
    spectra = dot(jnp.concatenate(parts, axis=1), gather) * pixels ** (-0.5)
    send_p[:, :, : 4 * comps] = spectra.astype(BF16).reshape(n, block, 4 * comps)
    back = exchange(send_p, recv_p, ps_sem, pr_sem)
    scale = (modes / cycles) ** 0.5 / jnp.sqrt(jnp.maximum(degree * (degree + 1.0), 1.0))
    f_level, f_eps, f_order = degree * scale, eps * scale, orders * scale
    for copy in back:
        copy.wait_recv()

    came = recv_p[...].reshape(n * block, LANES)[:, : 4 * comps].astype(F32).T.astype(BF16)
    by_pair = dot(came, place)
    first = jnp.concatenate([by_pair[: 2 * comps] * with_cos, by_pair[2 * comps :] * with_sin], 0)
    second = by_pair[: 2 * comps] * with_sin
    owner = div(iota((1, total), 1), span)
    keep = [jnp.where(owner == p, 1.0, 0.0) for p in range(pairs)]
    first = jnp.concatenate([(first * keep[p]).astype(BF16) for p in range(pairs)], axis=0)
    second = jnp.concatenate([(second * keep[p]).astype(BF16) for p in range(pairs)], axis=0)
    here = dot(first, leg_all[...])
    before = dot(second, prev_all[...])
    for p in range(pairs):
        a, b = 4 * comps * p, 2 * comps * p
        lev, ep, az = f_level[p : p + 1], f_eps[p : p + 1], f_order[p : p + 1]
        grad = (
            lev * here[a : a + comps] - ep * before[b : b + comps]
            + az * here[a + 2 * comps : a + 3 * comps]
        )
        curl = (
            lev * here[a + comps : a + 2 * comps] - ep * before[b + comps : b + 2 * comps]
            + az * here[a + 3 * comps : a + 4 * comps]
        )
        for s in range(sims):
            grad_ref[p, s] = grad[2 * s : 2 * s + 2]
            curl_ref[p, s] = curl[2 * s : 2 * s + 2]
    for copy in copies + back:
        copy.wait_send()


def fused(tbar_alm, twf_alm, legendre, m_slots, cycle_order, colatitude, cycle_weight, pixel_mask, n):
    pairs, sims, _, rows = tbar_alm.shape
    modes = rows - 1
    cycles = legendre.shape[2]
    pixels = pixel_mask.shape[1]
    total = pairs * 2 * cycles
    by_cycle = jnp.transpose(legendre, (0, 2, 1))
    table = jnp.asarray(split_tables(modes, pixels, sims))
    vmem, smem = pl.BlockSpec(memory_space=pltpu.VMEM), pl.BlockSpec(memory_space=pltpu.SMEM)
    out = jax.ShapeDtypeStruct(tbar_alm.shape, F32)
    return pl.pallas_call(
        functools.partial(fused_kernel, n, modes, rows, cycles, pixels, sims),
        out_shape=(out, out),
        in_specs=[smem] * 4 + [vmem] * 5 + [pl.BlockSpec(memory_space=pl.ANY)],
        out_specs=(vmem, vmem),
        scratch_shapes=[
            pltpu.VMEM(table.shape, BF16),
            pltpu.VMEM((total, rows), BF16),
            pltpu.VMEM((total, rows), BF16),
        ]
        + [pltpu.VMEM((n, 2 * pairs, LANES), BF16)] * 4
        + [pltpu.SemaphoreType.DMA]
        + [pltpu.SemaphoreType.DMA((n,))] * 4,
        compiler_params=pltpu.CompilerParams(collective_id=0, has_side_effects=True),
        name="estimator",
    )(
        m_slots, cycle_order, colatitude, cycle_weight, m_slots.reshape(1, -1), tbar_alm,
        twf_alm, by_cycle, pixel_mask.reshape(pixels // LANES, LANES), table,
    )


def body(n, *args):
    tbar_alm, legendre, pixel_mask = args[0], args[2], args[7]
    pairs, sims, _, rows = tbar_alm.shape
    cycles = legendre.shape[2]
    fits = (
        pairs == 8
        and cycles % 16 == 0
        and pixel_mask.shape[0] == 1
        and pairs * 2 * cycles <= 512
        and rows <= 1025
        and (pixel_mask.shape[1] // LANES * sims) % LANES == 0
        and sims % 4 == 0
        and all(v & (v - 1) == 0 for v in (sims, cycles, pixel_mask.shape[1]))
    )
    return fused(*args, n) if fits else shards(*args)


def solution(mesh):
    return jax.shard_map(
        functools.partial(body, mesh.shape["ma"]),
        mesh=mesh,
        in_specs=(
            P("ma", "grp", None, None),
            P("ma", "grp", None, None),
            P("ma", None, None),
            P(),
            P(),
            P(),
            P(),
            P("ma", None),
        ),
        out_specs=(P("ma", "grp", None, None), P("ma", "grp", None, None)),
        check_vma=False,
    )
```

```python
import math

import functools

import jax
import jax.numpy as jnp
import numpy as np
from jax import lax
from jax.experimental import pallas as pl
from jax.experimental.pallas import tpu as pltpu
from jax.sharding import PartitionSpec as P


def pair_layout(small_orders, mode_count):
    row_index = lax.broadcasted_iota(jnp.int32, (small_orders.shape[0], mode_count + 1), 1)
    smaller = small_orders[:, None]
    upper_half = row_index >= mode_count - smaller
    degree = jnp.where(upper_half, row_index - 1, smaller + row_index)
    orders = jnp.where(upper_half, mode_count - 1 - smaller, smaller + 0 * row_index)
    return (upper_half, degree.astype(jnp.float32), orders.astype(jnp.float32))


def raising(degree, orders):
    square = (
        (degree * degree - orders * orders)
        * (2.0 * degree + 1.0)
        / jnp.maximum(2.0 * degree - 1.0, 1.0)
    )
    return jnp.where(degree > orders, jnp.sqrt(jnp.where(degree > orders, square, 0.0)), 0.0)


def synthesis_sets(tbar_alm, twf_alm, degree, raising_factor, mode_count):
    wiener = twf_alm.astype(jnp.float32)
    scaled = (raising_factor / mode_count)[:, None, None, :] * wiener
    raised = jnp.concatenate([scaled[..., 1:], jnp.zeros_like(scaled[..., :1])], axis=-1)
    stacked = jnp.stack(
        [
            tbar_alm.astype(jnp.float32),
            wiener,
            (degree / mode_count)[:, None, None, :] * wiener,
            raised,
        ],
        axis=2,
    )
    return stacked.reshape(stacked.shape[0], stacked.shape[1], 8, stacked.shape[4]).astype(
        jnp.bfloat16
    )


def mode_columns(small_orders, mode_count):
    return jnp.stack([small_orders, mode_count - 1 - small_orders], axis=1).reshape(-1)


def fourier_table(orders_int, pixel_count):
    pixel_index = lax.broadcasted_iota(jnp.int32, (orders_int.shape[0], pixel_count), 1)
    turns = orders_int[:, None] * pixel_index % pixel_count
    radians = turns.astype(jnp.float32) * (2.0 * math.pi / pixel_count)
    return jnp.stack([jnp.cos(radians), -jnp.sin(radians)], axis=0).astype(jnp.bfloat16)


def combine_modes(legendre_sums, orders_int, cos_cycle, sin_cycle, mode_count):
    orders_real = orders_int.astype(jnp.float32)
    inv_sin = 1.0 / sin_cycle
    ratio = (orders_real / mode_count)[:, None]
    theta_real = (cos_cycle * legendre_sums[:, 4] - legendre_sums[:, 6]) * inv_sin
    theta_imag = (cos_cycle * legendre_sums[:, 5] - legendre_sums[:, 7]) * inv_sin
    phi_real = -ratio * legendre_sums[:, 3] * inv_sin
    phi_imag = ratio * legendre_sums[:, 2] * inv_sin
    weight = (jnp.where(orders_int == 0, 1.0, 2.0) * mode_count ** (-0.5))[:, None]
    stacked = jnp.stack(
        [legendre_sums[:, 0], legendre_sums[:, 1], theta_real, theta_imag, phi_real, phi_imag],
        axis=1,
    )
    return (stacked * weight).astype(jnp.bfloat16)


def analysis_sets(spectra, colatitude, cycle_weight):
    with_cos = cycle_weight * jnp.cos(colatitude) / jnp.sin(colatitude)
    with_sin = cycle_weight / jnp.sin(colatitude)
    stacked = jnp.stack(
        [
            spectra[:, 0] * with_cos,
            spectra[:, 0] * with_sin,
            spectra[:, 1] * with_cos,
            spectra[:, 1] * with_sin,
        ],
        axis=1,
    )
    return stacked.reshape(spectra.shape[0], 8, spectra.shape[3], spectra.shape[4]).astype(
        jnp.bfloat16
    )


def estimate(merged, degree, orders, raising_factor, mode_count, cycle_count):
    level = degree[:, None, :]
    azimuth = orders[:, None, :]
    factor = raising_factor[:, None, :]

    def previous(values):
        return jnp.concatenate([jnp.zeros_like(values[..., :1]), values[..., :-1]], axis=-1)

    grad_real = (
        level * merged[:, :, 0] - factor * previous(merged[:, :, 2]) + azimuth * merged[:, :, 7]
    )
    grad_imag = (
        level * merged[:, :, 1] - factor * previous(merged[:, :, 3]) - azimuth * merged[:, :, 6]
    )
    curl_real = (
        level * merged[:, :, 4] - factor * previous(merged[:, :, 6]) - azimuth * merged[:, :, 3]
    )
    curl_imag = (
        level * merged[:, :, 5] - factor * previous(merged[:, :, 7]) + azimuth * merged[:, :, 2]
    )
    scale = (mode_count / cycle_count) ** 0.5 / jnp.sqrt(jnp.maximum(level * (level + 1.0), 1.0))
    scale = scale[:, :, None, :]
    return (
        jnp.stack([grad_real, grad_imag], axis=2) * scale,
        jnp.stack([curl_real, curl_imag], axis=2) * scale,
    )


def shards(tbar_alm, twf_alm, legendre, m_slots, cycle_order, colatitude, cycle_weight, pixel_mask):
    pairs_dev = tbar_alm.shape[0]
    row_count = tbar_alm.shape[3]
    mode_count = row_count - 1
    cycle_count = legendre.shape[2]
    cycle_dev = pixel_mask.shape[0]
    pixel_count = pixel_mask.shape[1]
    device_slot = lax.axis_index("ma")
    local_small = lax.dynamic_slice_in_dim(m_slots, device_slot * pairs_dev, pairs_dev)
    upper_half, degree, orders = pair_layout(local_small, mode_count)
    raising_factor = raising(degree, orders)
    coeff_sets = synthesis_sets(tbar_alm, twf_alm, degree, raising_factor, mode_count)
    halves = jnp.stack([jnp.logical_not(upper_half), upper_half], axis=1)
    masked = coeff_sets[:, None] * halves.astype(jnp.bfloat16)[:, :, None, None, :]
    legendre_sums = jnp.einsum(
        "phsck,pkr->scphr", masked, legendre, preferred_element_type=jnp.float32
    )
    legendre_sums = jnp.take(legendre_sums, cycle_order, axis=4)
    legendre_sums = legendre_sums.reshape(legendre_sums.shape[0], 8, 2 * pairs_dev, cycle_count)
    all_orders = mode_columns(m_slots, mode_count)
    dft_table = fourier_table(all_orders, pixel_count)
    pixel_weights = pixel_mask.astype(jnp.float32)
    slot_theta = jnp.take(colatitude, cycle_order)
    local_orders = mode_columns(local_small, mode_count)
    outgoing = combine_modes(
        legendre_sums, local_orders, jnp.cos(slot_theta), jnp.sin(slot_theta), mode_count
    )
    fourier = lax.all_to_all(outgoing, "ma", split_axis=3, concat_axis=2, tiled=True)
    fourier = fourier.reshape(fourier.shape[0], 3, 2, mode_count, cycle_dev)
    cycle_maps = jnp.einsum(
        "sqemr,emj->sqrj", fourier, dft_table, preferred_element_type=jnp.float32
    )
    products = (pixel_weights * cycle_maps[:, 0:1] * cycle_maps[:, 1:3]).astype(jnp.bfloat16)
    spectra = jnp.einsum("sqrj,emj->sqemr", products, dft_table, preferred_element_type=jnp.float32)
    received = (spectra * pixel_count ** (-0.5)).astype(jnp.bfloat16)
    returned = lax.all_to_all(received, "ma", split_axis=3, concat_axis=4, tiled=True)
    inverse = (
        jnp.zeros((cycle_count,), jnp.int32).at[cycle_order].set(lax.iota(jnp.int32, cycle_count))
    )
    spectra = jnp.take(returned, inverse, axis=4).astype(jnp.float32)
    weighted = analysis_sets(spectra, colatitude, cycle_weight)
    weighted = weighted.reshape(weighted.shape[0], 8, pairs_dev, 2, cycle_count)
    projected = jnp.einsum(
        "scphr,pkr->phsck", weighted, legendre, preferred_element_type=jnp.float32
    )
    merged = jnp.sum(projected * halves.astype(jnp.float32)[:, :, None, None, :], axis=1)
    return estimate(merged, degree, orders, raising_factor, mode_count, cycle_count)


LANES = 128
F32 = jnp.float32
BF16 = jnp.bfloat16


def split_tables(mode_count, pixel_count, sims):
    m = np.arange(mode_count)[None, :]
    low = np.arange(LANES)[:, None]
    high = np.repeat(np.arange(pixel_count // LANES), sims)[:, None] * LANES
    fine = (m * low % pixel_count) * (2.0 * math.pi / pixel_count)
    coarse = (m * high % pixel_count) * (2.0 * math.pi / pixel_count)
    cos_high = np.cos(coarse).astype(np.float32)
    sin_high = np.sin(coarse).astype(np.float32)

    def halves(values):
        upper = values.astype(BF16)
        return upper, (values - upper.astype(np.float32)).astype(BF16)

    return np.concatenate(
        [np.cos(fine).astype(BF16), (-np.sin(fine)).astype(BF16)]
        + list(halves(cos_high))
        + list(halves(sin_high)),
        axis=0,
    )


def iota(shape, axis):
    return lax.broadcasted_iota(jnp.int32, shape, axis)


def div(values, size):
    return values >> (size.bit_length() - 1)


def mod(values, size):
    return values & (size - 1)


def one_hot(condition):
    return jnp.where(condition, 1.0, 0.0).astype(BF16)


def dot(left, right):
    return jnp.dot(left, right, preferred_element_type=F32)


def dot_t(left, right):
    return lax.dot_general(left, right, (((1,), (1,)), ((), ())), preferred_element_type=F32)


def fused_kernel(
    n, modes, rows, cycles, pixels, sims,
    slots_s, cycle_s, colat_s, weight_s, slots_v, tbar_ref, twf_ref, leg_ref, mask_ref,
    table_hbm, grad_ref, curl_ref,
    table_v, leg_all, prev_all, send_f, recv_f, send_p, recv_p,
    table_sem, fs_sem, fr_sem, ps_sem, pr_sem,
):
    me = lax.axis_index("ma")
    pairs, padded = tbar_ref.shape[0], rows
    block = 2 * pairs
    comps = 2 * sims
    span = 2 * cycles
    total = pairs * span
    fetch = pltpu.make_async_copy(table_hbm, table_v, table_sem)
    fetch.start()
    barrier = pltpu.get_barrier_semaphore()
    for off in range(1, n):
        pl.semaphore_signal(
            barrier, inc=1, device_id={"ma": lax.rem(me + off, n)},
            device_id_type=pl.DeviceIdType.MESH,
        )

    row_shape = (pairs, padded)
    smaller = jnp.zeros(row_shape, jnp.int32)
    for p in range(pairs):
        smaller = jnp.where(iota(row_shape, 0) == p, slots_s[me * pairs + p], smaller)
    k = iota(row_shape, 1)
    upper = k >= modes - smaller
    degree = jnp.where(upper, k - 1, smaller + k).astype(F32)
    orders = jnp.where(upper, modes - 1 - smaller, smaller).astype(F32)
    eps = raising(degree, orders)
    upper_f = jnp.where(upper, 1.0, 0.0)
    lower_f = 1.0 - upper_f

    colat = jnp.zeros((cycles, 4 * comps), F32)
    for r in range(cycles):
        colat = jnp.where(iota(colat.shape, 0) == r, colat_s[r], colat)
    csc = 1.0 / jnp.sin(colat)
    cot = jnp.cos(colat) * csc
    lane = iota(colat.shape, 1)
    group = div(lane, comps)
    part_a = jnp.where(group == 0, 1.0, jnp.where(group == 1, cot, 0.0))
    part_m = jnp.where(group == 2, csc, 0.0)
    part_b = jnp.where(group == 1, csc, 0.0)

    blank = jnp.zeros((comps, padded), F32)
    pieces = []
    for p in range(pairs):
        tbar = jnp.concatenate([tbar_ref[p, s].astype(F32) for s in range(sims)], axis=0)
        twf = jnp.concatenate([twf_ref[p, s].astype(F32) for s in range(sims)], axis=0)
        deg_p, eps_p = degree[p : p + 1] / modes, eps[p : p + 1] / modes
        sets_a = jnp.concatenate([tbar, deg_p * twf, twf, blank], axis=0)
        sets_b = jnp.concatenate([blank, -(eps_p * twf), blank, blank], axis=0)
        leg = leg_ref[p].astype(F32)
        prev = jnp.concatenate([jnp.zeros_like(leg[:, :1]), leg[:, : rows - 1]], axis=1)
        low, high = lower_f[p : p + 1], upper_f[p : p + 1]
        leg = jnp.concatenate([leg * low, leg * high], axis=0).astype(BF16)
        prev = jnp.concatenate([prev * low, prev * high], axis=0).astype(BF16)
        leg_all[pl.ds(p * span, span), :] = leg
        prev_all[pl.ds(p * span, span), :] = prev
        out_a = dot_t(leg, sets_a.astype(BF16))
        out_b = dot_t(prev, sets_b.astype(BF16))
        for h in range(2):
            small = slots_s[me * pairs + p]
            order = modes - 1 - small if h else small
            norm = jnp.where(order == 0, 1.0, 2.0) * modes ** (-0.5)
            ratio = order.astype(F32) / modes
            rng = slice(h * cycles, (h + 1) * cycles)
            pieces.append((out_a[rng] * (part_a + part_m * ratio) + out_b[rng] * part_b) * norm)
    fourier = jnp.concatenate(pieces, axis=0).astype(BF16)

    base_shape = (block, total)
    row = iota(base_shape, 0)
    base = iota(base_shape, 1) - (mod(row, pairs) * span + div(row, pairs) * cycles)
    place = jnp.concatenate(
        [jnp.where(base == cycle_s[i], 1.0, 0.0) for i in range(cycles)], axis=0
    ).astype(BF16)
    placed = dot(place, fourier).astype(BF16)
    send_f[:, :, : 4 * comps] = placed.reshape(n, block, 4 * comps)

    def exchange(send, recv, s_sem, r_sem):
        copies = []
        for off in range(1, n):
            to = lax.rem(me + off, n)
            copy = pltpu.make_async_remote_copy(
                src_ref=send.at[to], dst_ref=recv.at[me], send_sem=s_sem.at[off],
                recv_sem=r_sem.at[off], device_id={"ma": to},
                device_id_type=pl.DeviceIdType.MESH,
            )
            copy.start()
            copies.append(copy)
        recv[me] = send[me]
        return copies

    pl.semaphore_wait(barrier, n - 1)
    copies = exchange(send_f, recv_f, fs_sem, fr_sem)

    spread_shape = (slots_v.shape[1], n * block)
    col = iota(spread_shape, 1)
    spread = one_hot(
        iota(spread_shape, 0) == div(col, block) * pairs + mod(col, pairs)
    )
    slots = jnp.broadcast_to(slots_v[...], (8, slots_v.shape[1]))
    high_part = div(slots, 256).astype(F32)
    low_part = mod(slots, 256).astype(F32)
    picked = 256.0 * dot(high_part.astype(BF16), spread) + dot(low_part.astype(BF16), spread)
    flip = mod(iota(picked.shape, 1), block) >= pairs
    picked = jnp.where(flip, modes - 1.0 - picked, picked)[0:1]
    select = one_hot(iota((modes, n * block), 0).astype(F32) == picked)

    hs = pixels // LANES * sims
    fetch.wait()
    moved = dot(table_v[...], select)
    fine_cos, fine_sin = moved[:LANES], moved[LANES : 2 * LANES]
    at = 2 * LANES
    cos_t = moved[at : at + hs] + moved[at + hs : at + 2 * hs]
    sin_t = moved[at + 2 * hs : at + 3 * hs] + moved[at + 3 * hs : at + 4 * hs]
    cos_h, sin_h = cos_t.T, sin_t.T
    synth = jnp.concatenate([fine_cos, fine_sin], axis=1).astype(BF16)
    anal = jnp.concatenate([fine_cos.T, fine_sin.T], axis=0).astype(BF16)

    exp_shape = (4 * comps, 6 * hs)
    ecol = iota(exp_shape, 1)
    which = div(ecol, hs)
    comp_q, comp_c = div(which, 2), mod(which, 2)
    source_c = jnp.where(comp_q == 2, 1 - comp_c, comp_c)
    hit = iota(exp_shape, 0) == comp_q * comps + 2 * mod(ecol, sims) + source_c
    sign = jnp.where(jnp.logical_and(comp_q == 2, comp_c == 0), -1.0, 1.0)
    expand = jnp.where(hit, sign, 0.0).astype(BF16)

    sel_shape = (4 * hs, 4 * comps)
    srow, scol = iota(sel_shape, 0), iota(sel_shape, 1)
    row_q, row_c = div(srow, 2 * hs), mod(div(srow, hs), 2)
    out_g, out_c = div(scol, comps), mod(scol, 2)
    want_q = jnp.where(jnp.logical_or(out_g == 1, out_g == 2), 1, 0)
    swap = out_g >= 2
    want_c = jnp.where(swap, 1 - out_c, out_c)
    same_s = mod(srow, sims) == div(mod(scol, comps), 2)
    negative = jnp.logical_or(
        jnp.logical_and(out_g == 2, out_c == 1), jnp.logical_and(out_g == 3, out_c == 0)
    )
    hit = jnp.logical_and(jnp.logical_and(row_q == want_q, row_c == want_c), same_s)
    gather = jnp.where(hit, jnp.where(negative, -1.0, 1.0), 0.0).astype(BF16)

    mask_t = mask_ref[...].astype(F32).T.astype(BF16)
    m_shape = (pixels // LANES, hs)
    mask = dot(mask_t, one_hot(iota(m_shape, 0) == div(iota(m_shape, 1), sims)))

    lane_shape = (8, total)
    cyc = mod(iota(lane_shape, 1), cycles)
    theta_l = jnp.zeros(lane_shape, F32)
    weight_l = jnp.zeros(lane_shape, F32)
    for r in range(cycles):
        theta_l = jnp.where(cyc == r, colat_s[r], theta_l)
        weight_l = jnp.where(cyc == r, weight_s[r], weight_l)
    with_sin = (weight_l / jnp.sin(theta_l))[0:1]
    with_cos = (weight_l * jnp.cos(theta_l) / jnp.sin(theta_l))[0:1]

    for copy in copies:
        copy.wait_recv()
    got = recv_f[...].reshape(n * block, LANES)[:, : 4 * comps]
    spread_f = dot(got, expand)
    real, imag = [], []
    for q in range(3):
        re = spread_f[:, 2 * q * hs : (2 * q + 1) * hs]
        im = spread_f[:, (2 * q + 1) * hs : (2 * q + 2) * hs]
        real.append((re * cos_h - im * sin_h).astype(BF16))
        imag.append((re * sin_h + im * cos_h).astype(BF16))
    turned = jnp.concatenate(
        [jnp.concatenate(real, axis=1), jnp.concatenate(imag, axis=1)], axis=0
    )
    maps = dot(synth, turned)
    lead = mask * maps[:, :hs]
    products = jnp.concatenate(
        [lead * maps[:, hs : 2 * hs], lead * maps[:, 2 * hs :]], axis=1
    ).astype(BF16)
    half = dot(anal, products)
    parts = []
    count = n * block
    for q in range(2):
        c_part = half[:count, q * hs : (q + 1) * hs]
        s_part = half[count:, q * hs : (q + 1) * hs]
        parts.append((cos_h * c_part + sin_h * s_part).astype(BF16))
        parts.append((cos_h * s_part - sin_h * c_part).astype(BF16))
    spectra = dot(jnp.concatenate(parts, axis=1), gather) * pixels ** (-0.5)
    send_p[:, :, : 4 * comps] = spectra.astype(BF16).reshape(n, block, 4 * comps)
    back = exchange(send_p, recv_p, ps_sem, pr_sem)
    scale = (modes / cycles) ** 0.5 / jnp.sqrt(jnp.maximum(degree * (degree + 1.0), 1.0))
    f_level, f_eps, f_order = degree * scale, eps * scale, orders * scale
    for copy in back:
        copy.wait_recv()

    came = recv_p[...].reshape(n * block, LANES)[:, : 4 * comps].astype(F32).T.astype(BF16)
    by_pair = dot(came, place)
    first = jnp.concatenate([by_pair[: 2 * comps] * with_cos, by_pair[2 * comps :] * with_sin], 0)
    second = by_pair[: 2 * comps] * with_sin
    owner = div(iota((1, total), 1), span)
    keep = [jnp.where(owner == p, 1.0, 0.0) for p in range(pairs)]
    first = jnp.concatenate([(first * keep[p]).astype(BF16) for p in range(pairs)], axis=0)
    second = jnp.concatenate([(second * keep[p]).astype(BF16) for p in range(pairs)], axis=0)
    here = dot(first, leg_all[...])
    before = dot(second, prev_all[...])
    for p in range(pairs):
        a, b = 4 * comps * p, 2 * comps * p
        lev, ep, az = f_level[p : p + 1], f_eps[p : p + 1], f_order[p : p + 1]
        grad = (
            lev * here[a : a + comps] - ep * before[b : b + comps]
            + az * here[a + 2 * comps : a + 3 * comps]
        )
        curl = (
            lev * here[a + comps : a + 2 * comps] - ep * before[b + comps : b + 2 * comps]
            + az * here[a + 3 * comps : a + 4 * comps]
        )
        for s in range(sims):
            grad_ref[p, s] = grad[2 * s : 2 * s + 2]
            curl_ref[p, s] = curl[2 * s : 2 * s + 2]
    for copy in copies + back:
        copy.wait_send()


def fused(tbar_alm, twf_alm, legendre, m_slots, cycle_order, colatitude, cycle_weight, pixel_mask, n):
    pairs, sims, _, rows = tbar_alm.shape
    modes = rows - 1
    cycles = legendre.shape[2]
    pixels = pixel_mask.shape[1]
    total = pairs * 2 * cycles
    by_cycle = jnp.transpose(legendre, (0, 2, 1))
    table = jnp.asarray(split_tables(modes, pixels, sims))
    vmem, smem = pl.BlockSpec(memory_space=pltpu.VMEM), pl.BlockSpec(memory_space=pltpu.SMEM)
    out = pltpu.VMEM(tbar_alm.shape, F32)
    return pl.pallas_call(
        functools.partial(fused_kernel, n, modes, rows, cycles, pixels, sims),
        out_shape=(out, out),
        in_specs=[smem] * 4 + [vmem] * 5 + [pl.BlockSpec(memory_space=pl.ANY)],
        out_specs=(vmem, vmem),
        scratch_shapes=[
            pltpu.VMEM(table.shape, BF16),
            pltpu.VMEM((total, rows), BF16),
            pltpu.VMEM((total, rows), BF16),
        ]
        + [pltpu.VMEM((n, 2 * pairs, LANES), BF16)] * 4
        + [pltpu.SemaphoreType.DMA]
        + [pltpu.SemaphoreType.DMA((n,))] * 4,
        compiler_params=pltpu.CompilerParams(collective_id=0, has_side_effects=True),
        name="estimator",
    )(
        m_slots, cycle_order, colatitude, cycle_weight, m_slots.reshape(1, -1), tbar_alm,
        twf_alm, by_cycle, pixel_mask.reshape(pixels // LANES, LANES), table,
    )


def body(n, *args):
    tbar_alm, legendre, pixel_mask = args[0], args[2], args[7]
    pairs, sims, _, rows = tbar_alm.shape
    cycles = legendre.shape[2]
    fits = (
        pairs == 8
        and cycles % 16 == 0
        and pixel_mask.shape[0] == 1
        and pairs * 2 * cycles <= 512
        and rows <= 1025
        and (pixel_mask.shape[1] // LANES * sims) % LANES == 0
        and sims % 4 == 0
        and all(v & (v - 1) == 0 for v in (sims, cycles, pixel_mask.shape[1]))
    )
    return fused(*args, n) if fits else shards(*args)


def solution(mesh):
    return jax.shard_map(
        functools.partial(body, mesh.shape["ma"]),
        mesh=mesh,
        in_specs=(
            P("ma", "grp", None, None),
            P("ma", "grp", None, None),
            P("ma", None, None),
            P(),
            P(),
            P(),
            P(),
            P("ma", None),
        ),
        out_specs=(P("ma", "grp", None, None), P("ma", "grp", None, None)),
        check_vma=False,
    )
```

```python
import math

import functools

import jax
import jax.numpy as jnp
import numpy as np
from jax import lax
from jax.experimental import pallas as pl
from jax.experimental.pallas import tpu as pltpu
from jax.sharding import PartitionSpec as P


def pair_layout(small_orders, mode_count):
    row_index = lax.broadcasted_iota(jnp.int32, (small_orders.shape[0], mode_count + 1), 1)
    smaller = small_orders[:, None]
    upper_half = row_index >= mode_count - smaller
    degree = jnp.where(upper_half, row_index - 1, smaller + row_index)
    orders = jnp.where(upper_half, mode_count - 1 - smaller, smaller + 0 * row_index)
    return (upper_half, degree.astype(jnp.float32), orders.astype(jnp.float32))


def raising(degree, orders):
    square = (
        (degree * degree - orders * orders)
        * (2.0 * degree + 1.0)
        / jnp.maximum(2.0 * degree - 1.0, 1.0)
    )
    return jnp.where(degree > orders, jnp.sqrt(jnp.where(degree > orders, square, 0.0)), 0.0)


def synthesis_sets(tbar_alm, twf_alm, degree, raising_factor, mode_count):
    wiener = twf_alm.astype(jnp.float32)
    scaled = (raising_factor / mode_count)[:, None, None, :] * wiener
    raised = jnp.concatenate([scaled[..., 1:], jnp.zeros_like(scaled[..., :1])], axis=-1)
    stacked = jnp.stack(
        [
            tbar_alm.astype(jnp.float32),
            wiener,
            (degree / mode_count)[:, None, None, :] * wiener,
            raised,
        ],
        axis=2,
    )
    return stacked.reshape(stacked.shape[0], stacked.shape[1], 8, stacked.shape[4]).astype(
        jnp.bfloat16
    )


def mode_columns(small_orders, mode_count):
    return jnp.stack([small_orders, mode_count - 1 - small_orders], axis=1).reshape(-1)


def fourier_table(orders_int, pixel_count):
    pixel_index = lax.broadcasted_iota(jnp.int32, (orders_int.shape[0], pixel_count), 1)
    turns = orders_int[:, None] * pixel_index % pixel_count
    radians = turns.astype(jnp.float32) * (2.0 * math.pi / pixel_count)
    return jnp.stack([jnp.cos(radians), -jnp.sin(radians)], axis=0).astype(jnp.bfloat16)


def combine_modes(legendre_sums, orders_int, cos_cycle, sin_cycle, mode_count):
    orders_real = orders_int.astype(jnp.float32)
    inv_sin = 1.0 / sin_cycle
    ratio = (orders_real / mode_count)[:, None]
    theta_real = (cos_cycle * legendre_sums[:, 4] - legendre_sums[:, 6]) * inv_sin
    theta_imag = (cos_cycle * legendre_sums[:, 5] - legendre_sums[:, 7]) * inv_sin
    phi_real = -ratio * legendre_sums[:, 3] * inv_sin
    phi_imag = ratio * legendre_sums[:, 2] * inv_sin
    weight = (jnp.where(orders_int == 0, 1.0, 2.0) * mode_count ** (-0.5))[:, None]
    stacked = jnp.stack(
        [legendre_sums[:, 0], legendre_sums[:, 1], theta_real, theta_imag, phi_real, phi_imag],
        axis=1,
    )
    return (stacked * weight).astype(jnp.bfloat16)


def analysis_sets(spectra, colatitude, cycle_weight):
    with_cos = cycle_weight * jnp.cos(colatitude) / jnp.sin(colatitude)
    with_sin = cycle_weight / jnp.sin(colatitude)
    stacked = jnp.stack(
        [
            spectra[:, 0] * with_cos,
            spectra[:, 0] * with_sin,
            spectra[:, 1] * with_cos,
            spectra[:, 1] * with_sin,
        ],
        axis=1,
    )
    return stacked.reshape(spectra.shape[0], 8, spectra.shape[3], spectra.shape[4]).astype(
        jnp.bfloat16
    )


def estimate(merged, degree, orders, raising_factor, mode_count, cycle_count):
    level = degree[:, None, :]
    azimuth = orders[:, None, :]
    factor = raising_factor[:, None, :]

    def previous(values):
        return jnp.concatenate([jnp.zeros_like(values[..., :1]), values[..., :-1]], axis=-1)

    grad_real = (
        level * merged[:, :, 0] - factor * previous(merged[:, :, 2]) + azimuth * merged[:, :, 7]
    )
    grad_imag = (
        level * merged[:, :, 1] - factor * previous(merged[:, :, 3]) - azimuth * merged[:, :, 6]
    )
    curl_real = (
        level * merged[:, :, 4] - factor * previous(merged[:, :, 6]) - azimuth * merged[:, :, 3]
    )
    curl_imag = (
        level * merged[:, :, 5] - factor * previous(merged[:, :, 7]) + azimuth * merged[:, :, 2]
    )
    scale = (mode_count / cycle_count) ** 0.5 / jnp.sqrt(jnp.maximum(level * (level + 1.0), 1.0))
    scale = scale[:, :, None, :]
    return (
        jnp.stack([grad_real, grad_imag], axis=2) * scale,
        jnp.stack([curl_real, curl_imag], axis=2) * scale,
    )


def shards(tbar_alm, twf_alm, legendre, m_slots, cycle_order, colatitude, cycle_weight, pixel_mask):
    pairs_dev = tbar_alm.shape[0]
    row_count = tbar_alm.shape[3]
    mode_count = row_count - 1
    cycle_count = legendre.shape[2]
    cycle_dev = pixel_mask.shape[0]
    pixel_count = pixel_mask.shape[1]
    device_slot = lax.axis_index("ma")
    local_small = lax.dynamic_slice_in_dim(m_slots, device_slot * pairs_dev, pairs_dev)
    upper_half, degree, orders = pair_layout(local_small, mode_count)
    raising_factor = raising(degree, orders)
    coeff_sets = synthesis_sets(tbar_alm, twf_alm, degree, raising_factor, mode_count)
    halves = jnp.stack([jnp.logical_not(upper_half), upper_half], axis=1)
    masked = coeff_sets[:, None] * halves.astype(jnp.bfloat16)[:, :, None, None, :]
    legendre_sums = jnp.einsum(
        "phsck,pkr->scphr", masked, legendre, preferred_element_type=jnp.float32
    )
    legendre_sums = jnp.take(legendre_sums, cycle_order, axis=4)
    legendre_sums = legendre_sums.reshape(legendre_sums.shape[0], 8, 2 * pairs_dev, cycle_count)
    all_orders = mode_columns(m_slots, mode_count)
    dft_table = fourier_table(all_orders, pixel_count)
    pixel_weights = pixel_mask.astype(jnp.float32)
    slot_theta = jnp.take(colatitude, cycle_order)
    local_orders = mode_columns(local_small, mode_count)
    outgoing = combine_modes(
        legendre_sums, local_orders, jnp.cos(slot_theta), jnp.sin(slot_theta), mode_count
    )
    fourier = lax.all_to_all(outgoing, "ma", split_axis=3, concat_axis=2, tiled=True)
    fourier = fourier.reshape(fourier.shape[0], 3, 2, mode_count, cycle_dev)
    cycle_maps = jnp.einsum(
        "sqemr,emj->sqrj", fourier, dft_table, preferred_element_type=jnp.float32
    )
    products = (pixel_weights * cycle_maps[:, 0:1] * cycle_maps[:, 1:3]).astype(jnp.bfloat16)
    spectra = jnp.einsum("sqrj,emj->sqemr", products, dft_table, preferred_element_type=jnp.float32)
    received = (spectra * pixel_count ** (-0.5)).astype(jnp.bfloat16)
    returned = lax.all_to_all(received, "ma", split_axis=3, concat_axis=4, tiled=True)
    inverse = (
        jnp.zeros((cycle_count,), jnp.int32).at[cycle_order].set(lax.iota(jnp.int32, cycle_count))
    )
    spectra = jnp.take(returned, inverse, axis=4).astype(jnp.float32)
    weighted = analysis_sets(spectra, colatitude, cycle_weight)
    weighted = weighted.reshape(weighted.shape[0], 8, pairs_dev, 2, cycle_count)
    projected = jnp.einsum(
        "scphr,pkr->phsck", weighted, legendre, preferred_element_type=jnp.float32
    )
    merged = jnp.sum(projected * halves.astype(jnp.float32)[:, :, None, None, :], axis=1)
    return estimate(merged, degree, orders, raising_factor, mode_count, cycle_count)


LANES = 128
F32 = jnp.float32
BF16 = jnp.bfloat16


def split_tables(mode_count, pixel_count, sims):
    m = np.arange(mode_count)[None, :]
    low = np.arange(LANES)[:, None]
    high = np.repeat(np.arange(pixel_count // LANES), sims)[:, None] * LANES
    fine = (m * low % pixel_count) * (2.0 * math.pi / pixel_count)
    coarse = (m * high % pixel_count) * (2.0 * math.pi / pixel_count)
    cos_high = np.cos(coarse).astype(np.float32)
    sin_high = np.sin(coarse).astype(np.float32)

    def halves(values):
        upper = values.astype(BF16)
        return upper, (values - upper.astype(np.float32)).astype(BF16)

    return np.concatenate(
        [np.cos(fine).astype(BF16), (-np.sin(fine)).astype(BF16)]
        + list(halves(cos_high))
        + list(halves(sin_high)),
        axis=0,
    )


def iota(shape, axis):
    return lax.broadcasted_iota(jnp.int32, shape, axis)


def div(values, size):
    return values >> (size.bit_length() - 1)


def mod(values, size):
    return values & (size - 1)


def one_hot(condition):
    return jnp.where(condition, 1.0, 0.0).astype(BF16)


def dot(left, right):
    return jnp.dot(left, right, preferred_element_type=F32)


def dot_t(left, right):
    return lax.dot_general(left, right, (((1,), (1,)), ((), ())), preferred_element_type=F32)


def fused_kernel(
    n, modes, rows, cycles, pixels, sims,
    slots_s, cycle_s, colat_s, weight_s, slots_v, tbar_hbm, twf_hbm, leg_hbm, mask_hbm,
    table_hbm, grad_ref, curl_ref, tbar_ref, twf_ref, leg_ref, mask_ref, table_v, leg_all, prev_all, send_f, recv_f, send_p, recv_p,
    load_sem, fs_sem, fr_sem, ps_sem, pr_sem,
):
    me = lax.axis_index("ma")
    pairs, padded = tbar_ref.shape[0], rows
    block = 2 * pairs
    comps = 2 * sims
    span = 2 * cycles
    total = pairs * span
    barrier = pltpu.get_barrier_semaphore()
    for off in range(1, n):
        pl.semaphore_signal(
            barrier, inc=1, device_id={"ma": lax.rem(me + off, n)},
            device_id_type=pl.DeviceIdType.MESH,
        )

    loads = [
        pltpu.make_async_copy(source, target, load_sem.at[at])
        for at, (source, target) in enumerate(
            [(leg_hbm, leg_ref), (tbar_hbm, tbar_ref), (twf_hbm, twf_ref),
             (table_hbm, table_v), (mask_hbm, mask_ref)]
        )
    ]
    for load in loads:
        load.start()

    row_shape = (pairs, padded)
    smaller = jnp.zeros(row_shape, jnp.int32)
    for p in range(pairs):
        smaller = jnp.where(iota(row_shape, 0) == p, slots_s[me * pairs + p], smaller)
    k = iota(row_shape, 1)
    upper = k >= modes - smaller
    degree = jnp.where(upper, k - 1, smaller + k).astype(F32)
    orders = jnp.where(upper, modes - 1 - smaller, smaller).astype(F32)
    eps = raising(degree, orders)
    upper_f = jnp.where(upper, 1.0, 0.0)
    lower_f = 1.0 - upper_f

    colat = jnp.zeros((cycles, 4 * comps), F32)
    for r in range(cycles):
        colat = jnp.where(iota(colat.shape, 0) == r, colat_s[r], colat)
    csc = 1.0 / jnp.sin(colat)
    cot = jnp.cos(colat) * csc
    lane = iota(colat.shape, 1)
    group = div(lane, comps)
    part_a = jnp.where(group == 0, 1.0, jnp.where(group == 1, cot, 0.0))
    part_m = jnp.where(group == 2, csc, 0.0)
    part_b = jnp.where(group == 1, csc, 0.0)

    blank = jnp.zeros((comps, padded), F32)
    pieces = []
    for load in loads[:3]:
        load.wait()
    for p in range(pairs):
        tbar = jnp.concatenate([tbar_ref[p, s].astype(F32) for s in range(sims)], axis=0)
        twf = jnp.concatenate([twf_ref[p, s].astype(F32) for s in range(sims)], axis=0)
        deg_p, eps_p = degree[p : p + 1] / modes, eps[p : p + 1] / modes
        sets_a = jnp.concatenate([tbar, deg_p * twf, twf, blank], axis=0)
        sets_b = jnp.concatenate([blank, -(eps_p * twf), blank, blank], axis=0)
        leg = leg_ref[p].astype(F32)
        prev = jnp.concatenate([jnp.zeros_like(leg[:, :1]), leg[:, : rows - 1]], axis=1)
        low, high = lower_f[p : p + 1], upper_f[p : p + 1]
        leg = jnp.concatenate([leg * low, leg * high], axis=0).astype(BF16)
        prev = jnp.concatenate([prev * low, prev * high], axis=0).astype(BF16)
        leg_all[pl.ds(p * span, span), :] = leg
        prev_all[pl.ds(p * span, span), :] = prev
        out_a = dot_t(leg, sets_a.astype(BF16))
        out_b = dot_t(prev, sets_b.astype(BF16))
        for h in range(2):
            small = slots_s[me * pairs + p]
            order = modes - 1 - small if h else small
            norm = jnp.where(order == 0, 1.0, 2.0) * modes ** (-0.5)
            ratio = order.astype(F32) / modes
            rng = slice(h * cycles, (h + 1) * cycles)
            pieces.append((out_a[rng] * (part_a + part_m * ratio) + out_b[rng] * part_b) * norm)
    fourier = jnp.concatenate(pieces, axis=0).astype(BF16)

    base_shape = (block, total)
    row = iota(base_shape, 0)
    base = iota(base_shape, 1) - (mod(row, pairs) * span + div(row, pairs) * cycles)
    place = jnp.concatenate(
        [jnp.where(base == cycle_s[i], 1.0, 0.0) for i in range(cycles)], axis=0
    ).astype(BF16)
    placed = dot(place, fourier).astype(BF16)
    send_f[:, :, : 4 * comps] = placed.reshape(n, block, 4 * comps)

    def exchange(send, recv, s_sem, r_sem):
        copies = []
        for off in range(1, n):
            to = lax.rem(me + off, n)
            copy = pltpu.make_async_remote_copy(
                src_ref=send.at[to], dst_ref=recv.at[me], send_sem=s_sem.at[off],
                recv_sem=r_sem.at[off], device_id={"ma": to},
                device_id_type=pl.DeviceIdType.MESH,
            )
            copy.start()
            copies.append(copy)
        recv[me] = send[me]
        return copies

    pl.semaphore_wait(barrier, n - 1)
    copies = exchange(send_f, recv_f, fs_sem, fr_sem)

    spread_shape = (slots_v.shape[1], n * block)
    col = iota(spread_shape, 1)
    spread = one_hot(
        iota(spread_shape, 0) == div(col, block) * pairs + mod(col, pairs)
    )
    slots = jnp.broadcast_to(slots_v[...], (8, slots_v.shape[1]))
    high_part = div(slots, 256).astype(F32)
    low_part = mod(slots, 256).astype(F32)
    picked = 256.0 * dot(high_part.astype(BF16), spread) + dot(low_part.astype(BF16), spread)
    flip = mod(iota(picked.shape, 1), block) >= pairs
    picked = jnp.where(flip, modes - 1.0 - picked, picked)[0:1]
    select = one_hot(iota((modes, n * block), 0).astype(F32) == picked)

    hs = pixels // LANES * sims
    for load in loads[3:]:
        load.wait()
    moved = dot(table_v[...], select)
    fine_cos, fine_sin = moved[:LANES], moved[LANES : 2 * LANES]
    at = 2 * LANES
    cos_t = moved[at : at + hs] + moved[at + hs : at + 2 * hs]
    sin_t = moved[at + 2 * hs : at + 3 * hs] + moved[at + 3 * hs : at + 4 * hs]
    cos_h, sin_h = cos_t.T, sin_t.T
    synth = jnp.concatenate([fine_cos, fine_sin], axis=1).astype(BF16)
    anal = jnp.concatenate([fine_cos.T, fine_sin.T], axis=0).astype(BF16)

    exp_shape = (4 * comps, 6 * hs)
    ecol = iota(exp_shape, 1)
    which = div(ecol, hs)
    comp_q, comp_c = div(which, 2), mod(which, 2)
    source_c = jnp.where(comp_q == 2, 1 - comp_c, comp_c)
    hit = iota(exp_shape, 0) == comp_q * comps + 2 * mod(ecol, sims) + source_c
    sign = jnp.where(jnp.logical_and(comp_q == 2, comp_c == 0), -1.0, 1.0)
    expand = jnp.where(hit, sign, 0.0).astype(BF16)

    sel_shape = (4 * hs, 4 * comps)
    srow, scol = iota(sel_shape, 0), iota(sel_shape, 1)
    row_q, row_c = div(srow, 2 * hs), mod(div(srow, hs), 2)
    out_g, out_c = div(scol, comps), mod(scol, 2)
    want_q = jnp.where(jnp.logical_or(out_g == 1, out_g == 2), 1, 0)
    swap = out_g >= 2
    want_c = jnp.where(swap, 1 - out_c, out_c)
    same_s = mod(srow, sims) == div(mod(scol, comps), 2)
    negative = jnp.logical_or(
        jnp.logical_and(out_g == 2, out_c == 1), jnp.logical_and(out_g == 3, out_c == 0)
    )
    hit = jnp.logical_and(jnp.logical_and(row_q == want_q, row_c == want_c), same_s)
    gather = jnp.where(hit, jnp.where(negative, -1.0, 1.0), 0.0).astype(BF16)

    mask_t = mask_ref[...].astype(F32).T.astype(BF16)
    m_shape = (pixels // LANES, hs)
    mask = dot(mask_t, one_hot(iota(m_shape, 0) == div(iota(m_shape, 1), sims)))

    lane_shape = (8, total)
    cyc = mod(iota(lane_shape, 1), cycles)
    theta_l = jnp.zeros(lane_shape, F32)
    weight_l = jnp.zeros(lane_shape, F32)
    for r in range(cycles):
        theta_l = jnp.where(cyc == r, colat_s[r], theta_l)
        weight_l = jnp.where(cyc == r, weight_s[r], weight_l)
    with_sin = (weight_l / jnp.sin(theta_l))[0:1]
    with_cos = (weight_l * jnp.cos(theta_l) / jnp.sin(theta_l))[0:1]

    for copy in copies:
        copy.wait_recv()
    got = recv_f[...].reshape(n * block, LANES)[:, : 4 * comps]
    spread_f = dot(got, expand)
    real, imag = [], []
    for q in range(3):
        re = spread_f[:, 2 * q * hs : (2 * q + 1) * hs]
        im = spread_f[:, (2 * q + 1) * hs : (2 * q + 2) * hs]
        real.append((re * cos_h - im * sin_h).astype(BF16))
        imag.append((re * sin_h + im * cos_h).astype(BF16))
    turned = jnp.concatenate(
        [jnp.concatenate(real, axis=1), jnp.concatenate(imag, axis=1)], axis=0
    )
    maps = dot(synth, turned)
    lead = mask * maps[:, :hs]
    products = jnp.concatenate(
        [lead * maps[:, hs : 2 * hs], lead * maps[:, 2 * hs :]], axis=1
    ).astype(BF16)
    half = dot(anal, products)
    parts = []
    count = n * block
    for q in range(2):
        c_part = half[:count, q * hs : (q + 1) * hs]
        s_part = half[count:, q * hs : (q + 1) * hs]
        parts.append((cos_h * c_part + sin_h * s_part).astype(BF16))
        parts.append((cos_h * s_part - sin_h * c_part).astype(BF16))
    spectra = dot(jnp.concatenate(parts, axis=1), gather) * pixels ** (-0.5)
    send_p[:, :, : 4 * comps] = spectra.astype(BF16).reshape(n, block, 4 * comps)
    back = exchange(send_p, recv_p, ps_sem, pr_sem)
    scale = (modes / cycles) ** 0.5 / jnp.sqrt(jnp.maximum(degree * (degree + 1.0), 1.0))
    f_level, f_eps, f_order = degree * scale, eps * scale, orders * scale
    for copy in back:
        copy.wait_recv()

    came = recv_p[...].reshape(n * block, LANES)[:, : 4 * comps].astype(F32).T.astype(BF16)
    by_pair = dot(came, place)
    first = jnp.concatenate([by_pair[: 2 * comps] * with_cos, by_pair[2 * comps :] * with_sin], 0)
    second = by_pair[: 2 * comps] * with_sin
    owner = div(iota((1, total), 1), span)
    keep = [jnp.where(owner == p, 1.0, 0.0) for p in range(pairs)]
    first = jnp.concatenate([(first * keep[p]).astype(BF16) for p in range(pairs)], axis=0)
    second = jnp.concatenate([(second * keep[p]).astype(BF16) for p in range(pairs)], axis=0)
    here = dot(first, leg_all[...])
    before = dot(second, prev_all[...])
    for p in range(pairs):
        a, b = 4 * comps * p, 2 * comps * p
        lev, ep, az = f_level[p : p + 1], f_eps[p : p + 1], f_order[p : p + 1]
        grad = (
            lev * here[a : a + comps] - ep * before[b : b + comps]
            + az * here[a + 2 * comps : a + 3 * comps]
        )
        curl = (
            lev * here[a + comps : a + 2 * comps] - ep * before[b + comps : b + 2 * comps]
            + az * here[a + 3 * comps : a + 4 * comps]
        )
        for s in range(sims):
            grad_ref[p, s] = grad[2 * s : 2 * s + 2]
            curl_ref[p, s] = curl[2 * s : 2 * s + 2]
    for copy in copies + back:
        copy.wait_send()


def fused(tbar_alm, twf_alm, legendre, m_slots, cycle_order, colatitude, cycle_weight, pixel_mask, n):
    pairs, sims, _, rows = tbar_alm.shape
    modes = rows - 1
    cycles = legendre.shape[2]
    pixels = pixel_mask.shape[1]
    total = pairs * 2 * cycles
    by_cycle = jnp.transpose(legendre, (0, 2, 1))
    table = jnp.asarray(split_tables(modes, pixels, sims))
    vmem, smem = pl.BlockSpec(memory_space=pltpu.VMEM), pl.BlockSpec(memory_space=pltpu.SMEM)
    out = pltpu.VMEM(tbar_alm.shape, F32)
    return pl.pallas_call(
        functools.partial(fused_kernel, n, modes, rows, cycles, pixels, sims),
        out_shape=(out, out),
        in_specs=[smem] * 4 + [vmem] + [pl.BlockSpec(memory_space=pl.ANY)] * 5,
        out_specs=(vmem, vmem),
        scratch_shapes=[
            pltpu.VMEM(tbar_alm.shape, BF16),
            pltpu.VMEM(twf_alm.shape, BF16),
            pltpu.VMEM(by_cycle.shape, BF16),
            pltpu.VMEM((pixels // LANES, LANES), jnp.int32),
            pltpu.VMEM(table.shape, BF16),
            pltpu.VMEM((total, rows), BF16),
            pltpu.VMEM((total, rows), BF16),
        ]
        + [pltpu.VMEM((n, 2 * pairs, LANES), BF16)] * 4
        + [pltpu.SemaphoreType.DMA((5,))]
        + [pltpu.SemaphoreType.DMA((n,))] * 4,
        compiler_params=pltpu.CompilerParams(collective_id=0, has_side_effects=True),
        name="estimator",
    )(
        m_slots, cycle_order, colatitude, cycle_weight, m_slots.reshape(1, -1), tbar_alm,
        twf_alm, by_cycle, pixel_mask.reshape(pixels // LANES, LANES), table,
    )


def body(n, *args):
    tbar_alm, legendre, pixel_mask = args[0], args[2], args[7]
    pairs, sims, _, rows = tbar_alm.shape
    cycles = legendre.shape[2]
    fits = (
        pairs == 8
        and cycles % 16 == 0
        and pixel_mask.shape[0] == 1
        and pairs * 2 * cycles <= 512
        and rows <= 1025
        and (pixel_mask.shape[1] // LANES * sims) % LANES == 0
        and sims % 4 == 0
        and all(v & (v - 1) == 0 for v in (sims, cycles, pixel_mask.shape[1]))
    )
    return fused(*args, n) if fits else shards(*args)


def solution(mesh):
    return jax.shard_map(
        functools.partial(body, mesh.shape["ma"]),
        mesh=mesh,
        in_specs=(
            P("ma", "grp", None, None),
            P("ma", "grp", None, None),
            P("ma", None, None),
            P(),
            P(),
            P(),
            P(),
            P("ma", None),
        ),
        out_specs=(P("ma", "grp", None, None), P("ma", "grp", None, None)),
        check_vma=False,
    )
```
